8 devices in a mesh: dp: 1 (over z), sp: 8 (over y, x, core).
Axes of the slice: x: 2, y: 2, z: 1, core: 2. Of those that a mesh axis runs over, the one named last changes fastest.
Arguments:
- tokens: bfloat16 [64, 2048], P('dp')
- positions: int32 [64], P('dp')
- k_cache: bfloat16 [64, 2048, 8, 128], P('dp', 'sp')
- v_cache: bfloat16 [64, 2048, 8, 128], P('dp', 'sp')
- w_q: bfloat16 [2048, 2048], replicated
- w_k: bfloat16 [2048, 1024], replicated
- w_v: bfloat16 [2048, 1024], replicated
- w_o: bfloat16 [2048, 2048], replicated
- attn_norm: bfloat16 [2048], replicated
- q_norm: bfloat16 [128], replicated
- k_norm: bfloat16 [128], replicated
Outputs:
- output 1: bfloat16 [64, 2048], P('dp')
- output 2: bfloat16 [64, 2048, 8, 128], P('dp', 'sp')
- output 3: bfloat16 [64, 2048, 8, 128], P('dp', 'sp')
- output 4: bfloat16 [64, 2, 8, 128], P('dp')
All inputs are finite; a program needn't handle non-finite values.
Results may differ from the reference program's by a relative error of at most 0.00659406.
Values sent between devices are 32-bit elements.
A program may use at most 1 GiB of HBM per device.

```python
import jax
import jax.numpy as jnp
from jax import lax

NUM_SEQS = 64
MODEL_DIM = 2048
Q_HEADS = 16
KV_HEADS = 8
HEAD_DIM = 128
CACHE_LEN = 2048

Q_PER_KV = Q_HEADS // KV_HEADS
NORM_EPS = 1e-6
ROPE_THETA = 1000000.0
NEG_FILL = -1e30


def setup_inputs(seed: int = 0, part: int = 0) -> dict:
    part_keys = jax.random.split(jax.random.fold_in(jax.random.key(seed), part), 5)
    shared = jax.random.split(jax.random.key(seed + 1), 7)
    cache_shape = (NUM_SEQS, CACHE_LEN, KV_HEADS, HEAD_DIM)
    tokens = jax.random.normal(part_keys[0], (NUM_SEQS, MODEL_DIM), jnp.float32)
    pos_draw = jax.random.randint(part_keys[1], (NUM_SEQS,), CACHE_LEN // 4, CACHE_LEN, dtype=jnp.int32)
    positions = pos_draw.at[0].set(CACHE_LEN - 1).at[1].set(CACHE_LEN // 4)
    k_cache = jax.random.normal(part_keys[2], cache_shape, jnp.float32)
    coarse = jax.random.normal(part_keys[3], (NUM_SEQS, 16, KV_HEADS, HEAD_DIM), jnp.float32)
    v_noise = jax.random.normal(part_keys[4], cache_shape, jnp.float32)
    v_cache = 1.5 * jnp.repeat(coarse, CACHE_LEN // 16, axis=1) + 0.5 * v_noise
    w_q = jax.random.normal(shared[0], (MODEL_DIM, Q_HEADS * HEAD_DIM), jnp.float32) * MODEL_DIM ** -0.5
    w_k = jax.random.normal(shared[1], (MODEL_DIM, KV_HEADS * HEAD_DIM), jnp.float32) * MODEL_DIM ** -0.5
    w_v = jax.random.normal(shared[2], (MODEL_DIM, KV_HEADS * HEAD_DIM), jnp.float32) * MODEL_DIM ** -0.5
    w_o = jax.random.normal(shared[3], (Q_HEADS * HEAD_DIM, MODEL_DIM), jnp.float32) * (Q_HEADS * HEAD_DIM) ** -0.5
    attn_norm = jax.random.uniform(shared[4], (MODEL_DIM,), jnp.float32, 0.5, 1.5)
    q_norm = jax.random.uniform(shared[5], (HEAD_DIM,), jnp.float32, 0.5, 2.0)
    k_norm = jax.random.uniform(shared[6], (HEAD_DIM,), jnp.float32, 0.5, 2.0)
    return {
        'tokens': tokens.astype(jnp.bfloat16),
        'positions': positions,
        'k_cache': k_cache.astype(jnp.bfloat16),
        'v_cache': v_cache.astype(jnp.bfloat16),
        'w_q': w_q.astype(jnp.bfloat16),
        'w_k': w_k.astype(jnp.bfloat16),
        'w_v': w_v.astype(jnp.bfloat16),
        'w_o': w_o.astype(jnp.bfloat16),
        'attn_norm': attn_norm.astype(jnp.bfloat16),
        'q_norm': q_norm.astype(jnp.bfloat16),
        'k_norm': k_norm.astype(jnp.bfloat16),
    }


def rms_scale(values, gain):
    return values * lax.rsqrt(jnp.mean(values * values, axis=-1, keepdims=True) + NORM_EPS) * gain.astype(jnp.float32)


def rope_table(positions):
    inv_freq = ROPE_THETA ** (-jnp.arange(HEAD_DIM // 2, dtype=jnp.float32) * 2.0 / HEAD_DIM)
    angles = positions.astype(jnp.float32)[:, None] * inv_freq[None, :]
    return jnp.cos(angles)[:, None, :], jnp.sin(angles)[:, None, :]


def norm_rope(proj, gain, cos_table, sin_table):
    normed = rms_scale(proj.astype(jnp.float32), gain)
    first_half = normed[..., :HEAD_DIM // 2]
    second_half = normed[..., HEAD_DIM // 2:]
    rotated = jnp.concatenate([first_half * cos_table - second_half * sin_table, second_half * cos_table + first_half * sin_table], axis=-1)
    return rotated.astype(jnp.bfloat16)


def reference(tokens, positions, k_cache, v_cache, w_q, w_k, w_v, w_o, attn_norm, q_norm, k_norm):
    tokens_f = tokens.astype(jnp.float32)
    hidden = rms_scale(tokens_f, attn_norm).astype(jnp.bfloat16)
    q_proj = jnp.dot(hidden, w_q, preferred_element_type=jnp.float32).astype(jnp.bfloat16).reshape(NUM_SEQS, Q_HEADS, HEAD_DIM)
    k_proj = jnp.dot(hidden, w_k, preferred_element_type=jnp.float32).astype(jnp.bfloat16).reshape(NUM_SEQS, KV_HEADS, HEAD_DIM)
    v_new = jnp.dot(hidden, w_v, preferred_element_type=jnp.float32).astype(jnp.bfloat16).reshape(NUM_SEQS, KV_HEADS, HEAD_DIM)
    cos_table, sin_table = rope_table(positions)
    q_rot = norm_rope(q_proj, q_norm, cos_table, sin_table)
    k_rot = norm_rope(k_proj, k_norm, cos_table, sin_table)
    slot_ids = jnp.arange(CACHE_LEN)
    write_mask = (slot_ids[None, :] == positions[:, None])[:, :, None, None]
    k_out = jnp.where(write_mask, k_rot[:, None], k_cache)
    v_out = jnp.where(write_mask, v_new[:, None], v_cache)
    score_scale = HEAD_DIM ** -0.5

    def one_seq(items):
        q_one, k_one, v_one, pos_one = items
        q_grp = q_one.reshape(KV_HEADS, Q_PER_KV, HEAD_DIM).astype(jnp.float32)
        scores = jnp.einsum('kgd,tkd->kgt', q_grp, k_one.astype(jnp.float32)) * score_scale
        live_mask = (slot_ids <= pos_one)[None, None, :]
        global_peak = jnp.max(jnp.where(live_mask, scores, NEG_FILL), axis=-1, keepdims=True)
        weights = jnp.where(live_mask, jnp.exp(scores - global_peak), 0.0)
        total_sum = jnp.sum(weights, axis=-1, keepdims=True)
        mixed = jnp.einsum('kgt,tkd->kgd', weights.astype(jnp.bfloat16).astype(jnp.float32), v_one.astype(jnp.float32))
        return (mixed / total_sum).astype(jnp.bfloat16).reshape(Q_HEADS * HEAD_DIM)

    attn_out = lax.map(one_seq, (q_rot, k_out, v_out, positions))
    block_out = (tokens_f + jnp.dot(attn_out, w_o, preferred_element_type=jnp.float32)).astype(jnp.bfloat16)
    new_kv = jnp.stack([k_rot, v_new], axis=1)
    return (block_out, k_out, v_out, new_kv)
```

```python
import jax
import jax.numpy as jnp
from jax import lax
from jax.experimental import pallas as pl
from jax.experimental.pallas import tpu as pltpu
from jax.sharding import PartitionSpec as P

NORM_EPS = 1e-6
ROPE_THETA = 1000000.0
NEG_FILL = -1e30
F32 = jnp.float32
BF16 = jnp.bfloat16

SEQS = 64
WIDTH = 2048
HEADS = 16
KV = 8
DIM = 128
SLOTS = 256
ROWS = SLOTS * KV
RANKS = 8
OWN = SEQS // RANKS
PART = OWN * HEADS + 8
CHUNK = 512
RING = 16
PAIRS = RING // 2
LAG = 3
MESH = pl.DeviceIdType.MESH


def rope_tables(positions):
    inv_freq = ROPE_THETA ** (-jnp.arange(DIM // 2, dtype=F32) * 2.0 / DIM)
    angles = positions.astype(F32)[:, None] * inv_freq[None, :]
    cos, sin = jnp.cos(angles), jnp.sin(angles)
    return jnp.concatenate([cos, cos], axis=-1), jnp.concatenate([-sin, sin], axis=-1)


def attend_kernel(pos_ref, tok_ref, cos_ref, sin_ref, an_ref, qn_ref, kn_ref, wq_ref, wk_ref, wv_ref, k_ref, v_ref,
                  part_ref, new_ref, ko_ref, vo_ref,
                  wbuf, hid, q_scr, kv_scr, key, stat, kbuf, vbuf, wsem, krs, vrs, kws, vws):
    start = lax.axis_index('sp') * SLOTS

    def weight_copy(c):
        if c < 4:
            src = wq_ref.at[:, pl.ds(c * CHUNK, CHUNK)]
        elif c < 6:
            src = wk_ref.at[:, pl.ds((c - 4) * CHUNK, CHUNK)]
        else:
            src = wv_ref.at[:, pl.ds((c - 6) * CHUNK, CHUNK)]
        return pltpu.make_async_copy(src, wbuf.at[c], wsem.at[c])

    def k_read(b):
        s = lax.rem(b, RING)
        return pltpu.make_async_copy(k_ref.at[b], kbuf.at[s], krs.at[s])

    def v_read(b):
        s = lax.rem(b, RING)
        return pltpu.make_async_copy(v_ref.at[b], vbuf.at[s], vrs.at[s])

    def k_write(b):
        s = lax.rem(b, RING)
        return pltpu.make_async_copy(kbuf.at[s], ko_ref.at[b], kws.at[s])

    def v_write(b):
        s = lax.rem(b, RING)
        return pltpu.make_async_copy(vbuf.at[s], vo_ref.at[b], vws.at[s])

    for c in range(8):
        weight_copy(c).start()

    def first_reads(b, carry):
        k_read(b).start()
        v_read(b).start()
        return carry

    lax.fori_loop(0, RING, first_reads, 0)

    x = tok_ref[...].astype(F32)
    scale = lax.rsqrt(jnp.mean(x * x, axis=-1, keepdims=True) + NORM_EPS)
    hid[...] = (x * scale * an_ref[...].astype(F32)).astype(BF16)
    row = lax.broadcasted_iota(jnp.int32, (HEADS, ROWS), 0)
    col = lax.broadcasted_iota(jnp.int32, (HEADS, ROWS), 1)
    key[...] = jnp.where((col & (KV - 1)) == (row >> 1), col, 1 << 30)

    def project(c):
        return jnp.dot(hid[...], wbuf[c], preferred_element_type=F32).astype(BF16).astype(F32)

    def norm_rope(y, gain):
        y = y * lax.rsqrt(jnp.mean(y * y, axis=-1, keepdims=True) + NORM_EPS) * gain
        return (y * cos_ref[...] + pltpu.roll(y, DIM // 2, 1) * sin_ref[...]).astype(BF16).astype(F32)

    qg = qn_ref[...].astype(F32)
    kg = kn_ref[...].astype(F32)
    for c in range(8):
        weight_copy(c).wait()
        y = project(c)
        for j in range(CHUNK // DIM):
            yh = y[:, j * DIM:(j + 1) * DIM]
            if c < 4:
                q_scr[pl.ds(c * 4 + j, SEQS, stride=HEADS), :] = norm_rope(yh, qg)
            elif c < 6:
                kv_scr[pl.ds((c - 4) * 4 + j, SEQS, stride=2 * KV), :] = norm_rope(yh, kg)
            else:
                kv_scr[pl.ds(KV + (c - 6) * 4 + j, SEQS, stride=2 * KV), :] = yh
    new_ref[...] = kv_scr[...].astype(BF16)

    row16 = lax.broadcasted_iota(jnp.int32, (16, DIM), 0)
    lane16 = lax.broadcasted_iota(jnp.int32, (HEADS, DIM), 1)

    def insert(buf, s, local, new):
        slot = jnp.clip(local, 0, SLOTS - 1)
        first = jnp.where(local == slot, (slot & 1) * KV, 64)
        block = pl.ds(pl.multiple_of((slot >> 1) * 16, 16), 16)
        both = jnp.concatenate([new, new], axis=0)
        old = buf[s, block, :].astype(F32)
        hit = (row16 >= first) & (row16 < first + KV)
        buf[s, block, :] = jnp.where(hit, both, old).astype(BF16)

    def attend(b):
        s = lax.rem(b, RING)
        local = pos_ref[b] - start
        q = q_scr[pl.ds(pl.multiple_of(b * HEADS, HEADS), HEADS), :].astype(BF16)
        scores = lax.dot_general(q, kbuf[s], (((1,), (1,)), ((), ())), preferred_element_type=F32) * (DIM ** -0.5)
        live = key[...] < (local + 1) * KV
        scores = jnp.where(live, scores, NEG_FILL)
        peak = jnp.max(scores, axis=-1, keepdims=True)
        e = jnp.where(live, jnp.exp(scores - peak), 0.0)
        total = jnp.sum(e, axis=-1, keepdims=True)
        out = jnp.dot(e.astype(BF16), vbuf[s], preferred_element_type=F32)
        return out, jnp.where(lane16 == 0, peak, total)

    def group(g, carry):
        def pair(j, carry):
            i = g * (OWN // 2) + j
            b0 = 2 * i

            @pl.when(i >= LAG)
            def _():
                for d in range(2):
                    old = b0 - 2 * LAG + d
                    k_write(old).wait()
                    v_write(old).wait()

            @pl.when((i >= LAG) & (i - LAG + PAIRS < SEQS // 2))
            def _():
                for d in range(2):
                    nxt = b0 - 2 * LAG + RING + d
                    k_read(nxt).start()
                    v_read(nxt).start()

            for d in range(2):
                k_read(b0 + d).wait()
                v_read(b0 + d).wait()
            for d in range(2):
                b = b0 + d
                s = lax.rem(b, RING)
                local = pos_ref[b] - start
                base = pl.multiple_of(b * 2 * KV, 2 * KV)
                insert(kbuf, s, local, kv_scr[pl.ds(base, KV), :])
                insert(vbuf, s, local, kv_scr[pl.ds(pl.multiple_of(base + KV, KV), KV), :])
            for d in range(2):
                out, st = attend(b0 + d)
                r = pl.multiple_of((2 * j + d) * HEADS, HEADS)
                part_ref[g, pl.ds(r, HEADS), :] = out
                stat[pl.ds(r, HEADS), :] = st
            for d in range(2):
                k_write(b0 + d).start()
                v_write(b0 + d).start()
            return carry

        lax.fori_loop(0, OWN // 2, pair, 0)
        part_ref[g, pl.ds(OWN * HEADS, 8), :] = stat[...].T[0:8, :]
        return carry

    lax.fori_loop(0, RANKS, group, 0)
    for b in range(SEQS - 2 * LAG, SEQS):
        k_write(b).wait()
        v_write(b).wait()


def combine_kernel(part_ref, tok_ref, wo_ref, out_ref, wobuf, recv, mixed, own, wsem, rs_send, rs_recv, ag_send, ag_recv):
    me = lax.axis_index('sp')
    cols = WIDTH // 4

    def wo_copy(c):
        return pltpu.make_async_copy(wo_ref.at[:, pl.ds(c * cols, cols)], wobuf.at[c], wsem.at[c])

    for c in range(4):
        wo_copy(c).start()

    barrier = pltpu.get_barrier_semaphore()
    for j in range(1, RANKS):
        pl.semaphore_signal(barrier, inc=1, device_id={'sp': lax.rem(me + j, RANKS)}, device_id_type=MESH)
    pl.semaphore_wait(barrier, RANKS - 1)

    def rs_copy(j):
        dst = lax.rem(me + j, RANKS)
        return pltpu.make_async_remote_copy(
            src_ref=part_ref.at[dst], dst_ref=recv.at[RANKS - j], send_sem=rs_send.at[j], recv_sem=rs_recv.at[RANKS - j],
            device_id={'sp': dst}, device_id_type=MESH)

    for j in range(1, RANKS):
        rs_copy(j).start()
    recv[0] = part_ref[me]
    for j in range(1, RANKS):
        rs_copy(j).wait()

    rows = OWN * HEADS
    stats = [recv[s, pl.ds(rows, 8), :].T for s in range(RANKS)]
    peaks = [st[:, 0:1] for st in stats]
    peak = peaks[0]
    for s in range(1, RANKS):
        peak = jnp.maximum(peak, peaks[s])
    total = jnp.zeros((rows, 1), F32)
    acc = jnp.zeros((rows, DIM), F32)
    for s in range(RANKS):
        w = jnp.exp(peaks[s] - peak)
        total = total + w * stats[s][:, 1:2]
        acc = acc + w * recv[s, pl.ds(0, rows), :]
    mixed[...] = acc / total
    attn = jnp.concatenate([mixed[pl.ds(h, OWN, stride=HEADS), :] for h in range(HEADS)], axis=1).astype(BF16)

    x = tok_ref[pl.ds(pl.multiple_of(me * OWN, OWN), OWN), :].astype(F32)

    def ag_copy(c, j):
        dst = lax.rem(me + j, RANKS)
        block = own.at[:, pl.ds(c * cols, cols)]
        return pltpu.make_async_remote_copy(
            src_ref=block, dst_ref=out_ref.at[pl.ds(pl.multiple_of(me * OWN, OWN), OWN), pl.ds(c * cols, cols)],
            send_sem=ag_send.at[c, j], recv_sem=ag_recv.at[c, RANKS - j], device_id={'sp': dst}, device_id_type=MESH)

    for c in range(4):
        wo_copy(c).wait()
        y = jnp.dot(attn, wobuf[c], preferred_element_type=F32) + x[:, c * cols:(c + 1) * cols]
        own[:, pl.ds(c * cols, cols)] = y
        for j in range(1, RANKS):
            ag_copy(c, j).start()
    out_ref[pl.ds(pl.multiple_of(me * OWN, OWN), OWN), :] = own[...]
    for c in range(4):
        for j in range(1, RANKS):
            ag_copy(c, j).wait()


def solution(mesh):
    cache_spec = P('dp', 'sp', None, None)
    hbm = pl.BlockSpec(memory_space=pltpu.HBM)
    vmem = pl.BlockSpec(memory_space=pltpu.VMEM)
    smem = pl.BlockSpec(memory_space=pltpu.SMEM)
    sds = jax.ShapeDtypeStruct

    def device_step(tokens, positions, k_cache, v_cache, w_q, w_k, w_v, w_o, attn_norm, q_norm, k_norm):
        cos, sin = rope_tables(positions)
        flat = (SEQS, ROWS, DIM)
        part, new, k_out, v_out = pl.pallas_call(
            attend_kernel,
            out_shape=(pltpu.VMEM((RANKS, PART, DIM), F32), sds((SEQS * 2 * KV, DIM), BF16), sds(flat, BF16), sds(flat, BF16)),
            in_specs=[smem] + [vmem] * 6 + [hbm] * 5,
            out_specs=(vmem, vmem, hbm, hbm),
            scratch_shapes=[
                pltpu.VMEM((8, WIDTH, CHUNK), BF16),
                pltpu.VMEM((SEQS, WIDTH), BF16),
                pltpu.VMEM((SEQS * HEADS, DIM), F32),
                pltpu.VMEM((SEQS * 2 * KV, DIM), F32),
                pltpu.VMEM((HEADS, ROWS), jnp.int32),
                pltpu.VMEM((OWN * HEADS, DIM), F32),
                pltpu.VMEM((RING, ROWS, DIM), BF16),
                pltpu.VMEM((RING, ROWS, DIM), BF16),
                pltpu.SemaphoreType.DMA((8,)),
                pltpu.SemaphoreType.DMA((RING,)),
                pltpu.SemaphoreType.DMA((RING,)),
                pltpu.SemaphoreType.DMA((RING,)),
                pltpu.SemaphoreType.DMA((RING,)),
            ],
            compiler_params=pltpu.CompilerParams(vmem_limit_bytes=56 << 20),
        )(positions, tokens, cos, sin, attn_norm.reshape(1, WIDTH), q_norm.reshape(1, DIM), k_norm.reshape(1, DIM),
          w_q, w_k, w_v, k_cache.reshape(flat), v_cache.reshape(flat))
        gathered = pl.pallas_call(
            combine_kernel,
            out_shape=sds((SEQS, WIDTH), F32),
            in_specs=[vmem, vmem, hbm],
            out_specs=vmem,
            scratch_shapes=[
                pltpu.VMEM((4, WIDTH, WIDTH // 4), BF16),
                pltpu.VMEM((RANKS, PART, DIM), F32),
                pltpu.VMEM((OWN * HEADS, DIM), F32),
                pltpu.VMEM((OWN, WIDTH), F32),
                pltpu.SemaphoreType.DMA((4,)),
                pltpu.SemaphoreType.DMA((RANKS,)),
                pltpu.SemaphoreType.DMA((RANKS,)),
                pltpu.SemaphoreType.DMA((4, RANKS)),
                pltpu.SemaphoreType.DMA((4, RANKS)),
            ],
            compiler_params=pltpu.CompilerParams(collective_id=0, has_side_effects=True, vmem_limit_bytes=40 << 20),
        )(part, tokens, pltpu.with_memory_space_constraint(w_o, pltpu.HBM))
        return gathered.astype(BF16), k_out.reshape(k_cache.shape), v_out.reshape(v_cache.shape), new.reshape(SEQS, 2, KV, DIM)

    return jax.shard_map(device_step, mesh=mesh, in_specs=(P('dp', None), P('dp'), cache_spec, cache_spec, P(), P(), P(), P(), P(), P(), P()), out_specs=(P('dp', None), cache_spec, cache_spec, P('dp', None, None, None)), check_vma=False)
```

```python
import functools

import jax
import jax.numpy as jnp
import numpy as np
from jax import lax
from jax.experimental import pallas as pl
from jax.experimental.pallas import tpu as pltpu
from jax.sharding import PartitionSpec as P

NORM_EPS = 1e-6
ROPE_THETA = 1000000.0
NEG_FILL = -1e30
F32 = jnp.float32
BF16 = jnp.bfloat16

SEQS = 64
WIDTH = 2048
HEADS = 16
KV = 8
DIM = 128
SLOTS = 256
ROWS = SLOTS * KV
RANKS = 8
OWN = SEQS // RANKS
PART = OWN * HEADS + 8
CHUNK = 512
RING = 12
PAIRS = RING // 2
LAG = 2
BOUNDS = (0, 8, 40, 64)
COLS = 512


def frequencies():
    half = ROPE_THETA ** (-np.arange(DIM // 2, dtype=np.float64) * 2.0 / DIM)
    return jnp.asarray(np.concatenate([half, half])[None, :], F32)


def attend_kernel(pos_ref, tok_ref, freq_ref, an_ref, qn_ref, kn_ref, wq_ref, wk_ref, wv_ref, k_ref, v_ref,
                  p0, p1, p2, p3, p4, p5, p6, p7, new_ref, ko_ref, vo_ref, keep_b, keep_c,
                  keep_a, wbuf, part_ref, hid, cos_scr, sin_scr, q_scr, kv_scr, key, stat, kbuf, wsem, krs, vrs, kws, vws):
    start = lax.axis_index('sp') * SLOTS

    def weight_copy(c):
        if c < 4:
            src = wq_ref.at[:, pl.ds(c * CHUNK, CHUNK)]
        elif c < 6:
            src = wk_ref.at[:, pl.ds((c - 4) * CHUNK, CHUNK)]
        else:
            src = wv_ref.at[:, pl.ds((c - 6) * CHUNK, CHUNK)]
        return pltpu.make_async_copy(src, wbuf.at[c], wsem.at[c])

    def k_read(b):
        s = lax.rem(b, RING)
        return pltpu.make_async_copy(k_ref.at[b], kbuf.at[s], krs.at[s])

    def v_copy(b, keep, first):
        s = lax.rem(b, RING)
        return pltpu.make_async_copy(v_ref.at[b], keep.at[b - first], vrs.at[s])

    def v_write(b):
        return pltpu.make_async_copy(keep_a.at[b], vo_ref.at[b], vws.at[b])

    keeps = (keep_a, keep_b, keep_c)

    def v_start(b):
        for keep, first, last in zip(keeps, BOUNDS, BOUNDS[1:]):
            @pl.when((b >= first) & (b < last))
            def _():
                v_copy(b, keep, first).start()

    def k_write(b):
        s = lax.rem(b, RING)
        return pltpu.make_async_copy(kbuf.at[s], ko_ref.at[b], kws.at[s])

    for c in range(8):
        weight_copy(c).start()

    def first_reads(b, carry):
        k_read(b).start()
        v_start(b)
        return carry

    lax.fori_loop(0, RING, first_reads, 0)

    x = tok_ref[...].astype(F32)
    scale = lax.rsqrt(jnp.mean(x * x, axis=-1, keepdims=True) + NORM_EPS)
    hid[...] = (x * scale * an_ref[...].astype(F32)[None, :]).astype(BF16)

    def fill(b, carry):
        cos_scr[pl.ds(b, 1), :] = jnp.full((1, DIM), pos_ref[b].astype(F32), F32)
        return carry

    lax.fori_loop(0, SEQS, fill, 0)
    angle = cos_scr[...] * freq_ref[...]
    lane = lax.broadcasted_iota(jnp.int32, (SEQS, DIM), 1)
    sin = jnp.sin(angle)
    cos_scr[...] = jnp.cos(angle)
    sin_scr[...] = jnp.where(lane < DIM // 2, -sin, sin)
    row = lax.broadcasted_iota(jnp.int32, (HEADS, ROWS), 0)
    col = lax.broadcasted_iota(jnp.int32, (HEADS, ROWS), 1)
    key[...] = jnp.where((col & (KV - 1)) == (row >> 1), col, 1 << 30)

    def project(c):
        return jnp.dot(hid[...], wbuf[c], preferred_element_type=F32).astype(BF16).astype(F32)

    def norm_rope(y, gain):
        y = y * lax.rsqrt(jnp.mean(y * y, axis=-1, keepdims=True) + NORM_EPS) * gain
        return (y * cos_scr[...] + pltpu.roll(y, DIM // 2, 1) * sin_scr[...]).astype(BF16).astype(F32)

    qg = qn_ref[...].astype(F32)[None, :]
    kg = kn_ref[...].astype(F32)[None, :]
    for c in range(8):
        weight_copy(c).wait()
        y = project(c)
        for j in range(CHUNK // DIM):
            yh = y[:, j * DIM:(j + 1) * DIM]
            if c < 4:
                q_scr[pl.ds(c * 4 + j, SEQS, stride=HEADS), :] = norm_rope(yh, qg)
            elif c < 6:
                kv_scr[pl.ds((c - 4) * 4 + j, SEQS, stride=2 * KV), :] = norm_rope(yh, kg)
            else:
                kv_scr[pl.ds(KV + (c - 6) * 4 + j, SEQS, stride=2 * KV), :] = yh
    new_ref[...] = kv_scr[...].astype(BF16)

    row16 = lax.broadcasted_iota(jnp.int32, (16, DIM), 0)
    lane16 = lax.broadcasted_iota(jnp.int32, (HEADS, DIM), 1)

    def insert(buf, s, local, new):
        slot = jnp.clip(local, 0, SLOTS - 1)
        first = jnp.where(local == slot, (slot & 1) * KV, 64)
        block = pl.ds(pl.multiple_of((slot >> 1) * 16, 16), 16)
        both = jnp.concatenate([new, new], axis=0)
        old = buf[s, block, :].astype(F32)
        hit = (row16 >= first) & (row16 < first + KV)
        buf[s, block, :] = jnp.where(hit, both, old).astype(BF16)

    def attend(b, keep, first):
        s = lax.rem(b, RING)
        local = pos_ref[b] - start
        q = q_scr[pl.ds(pl.multiple_of(b * HEADS, HEADS), HEADS), :].astype(BF16)
        scores = lax.dot_general(q, kbuf[s], (((1,), (1,)), ((), ())), preferred_element_type=F32) * (DIM ** -0.5)
        live = key[...] < (local + 1) * KV
        scores = jnp.where(live, scores, NEG_FILL)
        peak = jnp.max(scores, axis=-1, keepdims=True)
        e = jnp.where(live, jnp.exp(scores - peak), 0.0)
        total = jnp.sum(e, axis=-1, keepdims=True)
        out = jnp.dot(e.astype(BF16), keep[b - first], preferred_element_type=F32)
        return out, jnp.where(lane16 == 0, peak, total)

    def group(keep, first, g, carry):
        def pair(j, carry):
            i = g * (OWN // 2) + j
            b0 = 2 * i

            @pl.when(i >= LAG)
            def _():
                for d in range(2):
                    old = b0 - 2 * LAG + d
                    k_write(old).wait()

            @pl.when((i >= LAG) & (i - LAG + PAIRS < SEQS // 2))
            def _():
                for d in range(2):
                    nxt = b0 - 2 * LAG + RING + d
                    k_read(nxt).start()
                    v_start(nxt)

            for d in range(2):
                k_read(b0 + d).wait()
                v_copy(b0 + d, keep, first).wait()
            for d in range(2):
                b = b0 + d
                s = lax.rem(b, RING)
                local = pos_ref[b] - start
                base = pl.multiple_of(b * 2 * KV, 2 * KV)
                insert(kbuf, s, local, kv_scr[pl.ds(base, KV), :])
                insert(keep, b - first, local, kv_scr[pl.ds(pl.multiple_of(base + KV, KV), KV), :])
            for d in range(2):
                out, st = attend(b0 + d, keep, first)
                r = pl.multiple_of((2 * j + d) * HEADS, HEADS)
                part_ref[g, pl.ds(r, HEADS), :] = out
                stat[pl.ds(r, HEADS), :] = st
            for d in range(2):
                k_write(b0 + d).start()
                if first == 0:
                    v_write(b0 + d).start()
            return carry

        lax.fori_loop(0, OWN // 2, pair, 0)
        part_ref[g, pl.ds(OWN * HEADS, 8), :] = stat[...].T[0:8, :]
        return carry

    for keep, first, last in zip(keeps, BOUNDS, BOUNDS[1:]):
        lax.fori_loop(first // OWN, last // OWN, functools.partial(group, keep, first), 0)
    for b in range(SEQS - 2 * LAG, SEQS):
        k_write(b).wait()
    for b in range(BOUNDS[1]):
        v_write(b).wait()
    me = lax.axis_index('sp')
    for j, p in enumerate((p0, p1, p2, p3, p4, p5, p6, p7)):
        p[...] = part_ref[lax.rem(me + j, RANKS)]


def store(keep_ref, vo_ref, sem, first):
    def copy(b):
        return pltpu.make_async_copy(keep_ref.at[b], vo_ref.at[first + b], sem)

    def start(b, carry):
        copy(b).start()
        return carry

    def wait(b, carry):
        copy(b).wait()
        return carry

    lax.fori_loop(0, keep_ref.shape[0], start, 0)
    return lambda: lax.fori_loop(0, keep_ref.shape[0], wait, 0)


def store_first_kernel(keep_b, wo_ref, vo_in_ref, vo_ref, wobuf_ref, sem, wsem):
    def wo_copy(c):
        return pltpu.make_async_copy(wo_ref.at[:, pl.ds(c * COLS, COLS)], wobuf_ref.at[c], wsem)

    for c in range(WIDTH // COLS):
        wo_copy(c).start()
    finish = store(keep_b, vo_ref, sem, BOUNDS[1])
    for c in range(WIDTH // COLS):
        wo_copy(c).wait()
    finish()


def store_rest_kernel(keep_c, vo_in_ref, rows_ref, vo_ref, sem):
    store(keep_c, vo_ref, sem, BOUNDS[2])()


def combine_kernel(r0, r1, r2, r3, r4, r5, r6, r7, wo_ref, vo_ref, rows_ref, mixed):
    recv = (r0, r1, r2, r3, r4, r5, r6, r7)
    rows = OWN * HEADS
    stats = [r[pl.ds(rows, 8), :].T for r in recv]
    peaks = [st[:, 0:1] for st in stats]
    peak = peaks[0]
    for s in range(1, RANKS):
        peak = jnp.maximum(peak, peaks[s])
    total = jnp.zeros((rows, 1), F32)
    acc = jnp.zeros((rows, DIM), F32)
    for s in range(RANKS):
        w = jnp.exp(peaks[s] - peak)
        total = total + w * stats[s][:, 1:2]
        acc = acc + w * recv[s][pl.ds(0, rows), :]
    mixed[...] = acc / total
    attn = jnp.concatenate([mixed[pl.ds(h, OWN, stride=HEADS), :] for h in range(HEADS)], axis=1).astype(BF16)
    for c in range(WIDTH // COLS):
        rows_ref[:, pl.ds(c * COLS, COLS)] = jnp.dot(attn, wo_ref[c], preferred_element_type=F32)


def finish_kernel(y0, y1, y2, y3, y4, y5, y6, y7, tok_ref, vo_ref, out_ref, scr):
    me = lax.axis_index('sp')
    for j, y in enumerate((y0, y1, y2, y3, y4, y5, y6, y7)):
        owner = lax.rem(me + RANKS - j, RANKS)
        scr[pl.ds(pl.multiple_of(owner * OWN, OWN), OWN), :] = y[...]
    out_ref[...] = (tok_ref[...].astype(F32) + scr[...]).astype(BF16)


def solution(mesh):
    cache_spec = P('dp', 'sp', None, None)
    hbm = pl.BlockSpec(memory_space=pltpu.HBM)
    vmem = pl.BlockSpec(memory_space=pltpu.VMEM)
    smem = pl.BlockSpec(memory_space=pltpu.SMEM)
    sds = jax.ShapeDtypeStruct
    flat = (SEQS, ROWS, DIM)
    dma = pltpu.SemaphoreType.DMA

    def shifted(a, j):
        return lax.ppermute(a, 'sp', [(i, (i + j) % RANKS) for i in range(RANKS)])

    def in_vmem(a):
        return pltpu.with_memory_space_constraint(a, pltpu.VMEM)

    def in_hbm(a):
        return pltpu.with_memory_space_constraint(a, pltpu.HBM)

    def params(mib):
        return pltpu.CompilerParams(vmem_limit_bytes=mib << 20)

    def store_cost(count):
        return pl.CostEstimate(flops=count * 10 ** 8, bytes_accessed=count * ROWS * DIM * 4, transcendentals=0)

    def device_step(tokens, positions, k_cache, v_cache, w_q, w_k, w_v, w_o, attn_norm, q_norm, k_norm):
        *parts, new, k_out, v_out, keep_b, keep_c = pl.pallas_call(
            attend_kernel,
            out_shape=(pltpu.VMEM((PART, DIM), F32),) * RANKS + (sds((SEQS * 2 * KV, DIM), BF16), sds(flat, BF16), sds(flat, BF16),
                       *(pltpu.VMEM((b - a, ROWS, DIM), BF16) for a, b in zip(BOUNDS[1:], BOUNDS[2:]))),
            in_specs=[smem] + [vmem] * 5 + [hbm] * 5,
            out_specs=(vmem,) * RANKS + (vmem, hbm, hbm, vmem, vmem),
            scratch_shapes=[
                pltpu.VMEM((BOUNDS[1], ROWS, DIM), BF16),
                pltpu.VMEM((8, WIDTH, CHUNK), BF16),
                pltpu.VMEM((RANKS, PART, DIM), F32),
                pltpu.VMEM((SEQS, WIDTH), BF16),
                pltpu.VMEM((SEQS, DIM), F32),
                pltpu.VMEM((SEQS, DIM), F32),
                pltpu.VMEM((SEQS * HEADS, DIM), F32),
                pltpu.VMEM((SEQS * 2 * KV, DIM), F32),
                pltpu.VMEM((HEADS, ROWS), jnp.int32),
                pltpu.VMEM((OWN * HEADS, DIM), F32),
                pltpu.VMEM((RING, ROWS, DIM), BF16),
                dma((8,)), dma((RING,)), dma((RING,)), dma((RING,)), dma((BOUNDS[1],)),
            ],
            compiler_params=params(28 + BOUNDS[1] // 2),
        )(positions, tokens, frequencies(), attn_norm, q_norm, k_norm, w_q, w_k, w_v, k_cache.reshape(flat), v_cache.reshape(flat))
        recv = [parts[0]] + [shifted(parts[j], j) for j in range(1, RANKS)]
        v_out, wobuf = pl.pallas_call(
            store_first_kernel,
            out_shape=(sds(flat, BF16), pltpu.VMEM((WIDTH // COLS, WIDTH, COLS), BF16)),
            in_specs=[vmem, hbm, hbm],
            out_specs=(hbm, vmem),
            scratch_shapes=[dma, dma],
            input_output_aliases={2: 0},
            compiler_params=params(2),
            cost_estimate=store_cost(BOUNDS[2] - BOUNDS[1]),
        )(in_vmem(keep_b), in_hbm(w_o), v_out)
        rows = pl.pallas_call(
            combine_kernel,
            out_shape=pltpu.VMEM((OWN, WIDTH), F32),
            in_specs=[vmem] * (RANKS + 1) + [hbm],
            out_specs=vmem,
            scratch_shapes=[pltpu.VMEM((OWN * HEADS, DIM), F32)],
            compiler_params=params(4),
        )(*recv, in_vmem(wobuf), in_hbm(v_out))
        gathered = [rows] + [shifted(rows, j) for j in range(1, RANKS)]
        v_out = pl.pallas_call(
            store_rest_kernel,
            out_shape=sds(flat, BF16),
            in_specs=[vmem, hbm, vmem],
            out_specs=hbm,
            scratch_shapes=[dma],
            input_output_aliases={1: 0},
            compiler_params=params(2),
            cost_estimate=store_cost(SEQS - BOUNDS[2]),
        )(in_vmem(keep_c), v_out, rows)
        block_out = pl.pallas_call(
            finish_kernel,
            out_shape=sds((SEQS, WIDTH), BF16),
            in_specs=[vmem] * (RANKS + 1) + [hbm],
            out_specs=vmem,
            scratch_shapes=[pltpu.VMEM((SEQS, WIDTH), F32)],
            compiler_params=params(4),
        )(*gathered, tokens, in_hbm(v_out))
        return block_out, k_out.reshape(k_cache.shape), v_out.reshape(v_cache.shape), new.reshape(SEQS, 2, KV, DIM)

    return jax.shard_map(device_step, mesh=mesh, in_specs=(P('dp', None), P('dp'), cache_spec, cache_spec, P(), P(), P(), P(), P(), P(), P()), out_specs=(P('dp', None), cache_spec, cache_spec, P('dp', None, None, None)), check_vma=False)
```

```python
import jax
import jax.numpy as jnp
import numpy as np
from jax import lax
from jax.experimental import pallas as pl
from jax.experimental.pallas import tpu as pltpu
from jax.sharding import PartitionSpec as P

NORM_EPS = 1e-6
ROPE_THETA = 1000000.0
NEG_FILL = -1e30
F32 = jnp.float32
BF16 = jnp.bfloat16
MESH = pl.DeviceIdType.MESH

SEQS = 64
WIDTH = 2048
HEADS = 16
KV = 8
DIM = 128
SLOTS = 256
ROWS = SLOTS * KV
RANKS = 8
OWN = SEQS // RANKS
EARLY = 32
LATE = SEQS - EARLY
OWN_E = EARLY // RANKS
OWN_L = LATE // RANKS
PART_E = OWN_E * HEADS + 8
PART_L = OWN_L * HEADS + 8
CHUNK = 512
RING = 16
PAIRS = RING // 2
LAG = 3
COLS = 512
CHUNKS = WIDTH // COLS


def frequencies():
    half = ROPE_THETA ** (-np.arange(DIM // 2, dtype=np.float64) * 2.0 / DIM)
    return jnp.asarray(np.concatenate([half, half])[None, :], F32)


def head_columns():
    row = lax.broadcasted_iota(jnp.int32, (HEADS, ROWS), 0)
    col = lax.broadcasted_iota(jnp.int32, (HEADS, ROWS), 1)
    return jnp.where((col & (KV - 1)) == (row >> 1), col, 1 << 30)


def insert(buf, index, local, new):
    row = lax.broadcasted_iota(jnp.int32, (2 * KV, DIM), 0)
    slot = jnp.clip(local, 0, SLOTS - 1)
    first = jnp.where(local == slot, (slot & 1) * KV, 64)
    block = pl.ds(pl.multiple_of((slot >> 1) * 2 * KV, 2 * KV), 2 * KV)
    both = jnp.concatenate([new, new], axis=0)
    old = buf[index, block, :].astype(F32)
    hit = (row >= first) & (row < first + KV)
    buf[index, block, :] = jnp.where(hit, both, old).astype(BF16)


def scores_of(q, k):
    return lax.dot_general(q, k, (((1,), (1,)), ((), ())), preferred_element_type=F32) * (DIM ** -0.5)


def stat_tile(peak, total):
    lane = lax.broadcasted_iota(jnp.int32, (HEADS, DIM), 1)
    return jnp.where(lane == 0, peak, total)


def early_kernel(pos_ref, tok_ref, freq_ref, an_ref, qn_ref, kn_ref, wq_ref, wk_ref, wv_ref, k_ref, v_ref,
                 part_ref, q_scr, kv_scr, new_ref, ko_ref, vo_ref,
                 wbuf, hid, cos_scr, sin_scr, key, stat, kbuf, vbuf, wsem, krs, vrs, kws, vws):
    start = lax.axis_index('sp') * SLOTS

    def weight_copy(c):
        if c < 4:
            src = wq_ref.at[:, pl.ds(c * CHUNK, CHUNK)]
        elif c < 6:
            src = wk_ref.at[:, pl.ds((c - 4) * CHUNK, CHUNK)]
        else:
            src = wv_ref.at[:, pl.ds((c - 6) * CHUNK, CHUNK)]
        return pltpu.make_async_copy(src, wbuf.at[c], wsem.at[c])

    def reads(b):
        s = lax.rem(b, RING)
        return (pltpu.make_async_copy(k_ref.at[b], kbuf.at[s], krs.at[s]),
                pltpu.make_async_copy(v_ref.at[b], vbuf.at[s], vrs.at[s]))

    def writes(b):
        s = lax.rem(b, RING)
        return (pltpu.make_async_copy(kbuf.at[s], ko_ref.at[b], kws.at[s]),
                pltpu.make_async_copy(vbuf.at[s], vo_ref.at[b], vws.at[s]))

    for c in range(8):
        weight_copy(c).start()

    def first_reads(b, carry):
        for copy in reads(b):
            copy.start()
        return carry

    lax.fori_loop(0, RING, first_reads, 0)

    x = tok_ref[...].astype(F32)
    scale = lax.rsqrt(jnp.mean(x * x, axis=-1, keepdims=True) + NORM_EPS)
    hid[...] = (x * scale * an_ref[...].astype(F32)[None, :]).astype(BF16)

    def fill(b, carry):
        cos_scr[pl.ds(b, 1), :] = jnp.full((1, DIM), pos_ref[b].astype(F32), F32)
        return carry

    lax.fori_loop(0, SEQS, fill, 0)
    angle = cos_scr[...] * freq_ref[...]
    lane = lax.broadcasted_iota(jnp.int32, (SEQS, DIM), 1)
    sin = jnp.sin(angle)
    cos_scr[...] = jnp.cos(angle)
    sin_scr[...] = jnp.where(lane < DIM // 2, -sin, sin)
    key[...] = head_columns()

    def norm_rope(y, gain):
        y = y * lax.rsqrt(jnp.mean(y * y, axis=-1, keepdims=True) + NORM_EPS) * gain
        return (y * cos_scr[...] + pltpu.roll(y, DIM // 2, 1) * sin_scr[...]).astype(BF16).astype(F32)

    qg = qn_ref[...].astype(F32)[None, :]
    kg = kn_ref[...].astype(F32)[None, :]
    for c in range(8):
        weight_copy(c).wait()
        y = jnp.dot(hid[...], wbuf[c], preferred_element_type=F32).astype(BF16).astype(F32)
        for j in range(CHUNK // DIM):
            yh = y[:, j * DIM:(j + 1) * DIM]
            if c < 4:
                q_scr[pl.ds(c * 4 + j, SEQS, stride=HEADS), :] = norm_rope(yh, qg)
            elif c < 6:
                kv_scr[pl.ds((c - 4) * 4 + j, SEQS, stride=2 * KV), :] = norm_rope(yh, kg)
            else:
                kv_scr[pl.ds(KV + (c - 6) * 4 + j, SEQS, stride=2 * KV), :] = yh
    new_ref[...] = kv_scr[...].astype(BF16)

    def attend(b):
        s = lax.rem(b, RING)
        local = pos_ref[b] - start
        q = q_scr[pl.ds(pl.multiple_of(b * HEADS, HEADS), HEADS), :].astype(BF16)
        scores = scores_of(q, kbuf[s])
        live = key[...] < (local + 1) * KV
        scores = jnp.where(live, scores, NEG_FILL)
        peak = jnp.max(scores, axis=-1, keepdims=True)
        e = jnp.where(live, jnp.exp(scores - peak), 0.0)
        total = jnp.sum(e, axis=-1, keepdims=True)
        out = jnp.dot(e.astype(BF16), vbuf[s], preferred_element_type=F32)
        return out, stat_tile(peak, total)

    def group(g, carry):
        def pair(j, carry):
            i = g * (OWN_E // 2) + j
            b0 = 2 * i

            @pl.when(i >= LAG)
            def _():
                for d in range(2):
                    for copy in writes(b0 - 2 * LAG + d):
                        copy.wait()

            @pl.when((i >= LAG) & (i - LAG + PAIRS < EARLY // 2))
            def _():
                for d in range(2):
                    for copy in reads(b0 - 2 * LAG + RING + d):
                        copy.start()

            for d in range(2):
                for copy in reads(b0 + d):
                    copy.wait()
            for d in range(2):
                b = b0 + d
                s = lax.rem(b, RING)
                local = pos_ref[b] - start
                base = pl.multiple_of(b * 2 * KV, 2 * KV)
                insert(kbuf, s, local, kv_scr[pl.ds(base, KV), :])
                insert(vbuf, s, local, kv_scr[pl.ds(pl.multiple_of(base + KV, KV), KV), :])
            for d in range(2):
                out, st = attend(b0 + d)
                r = pl.multiple_of((2 * j + d) * HEADS, HEADS)
                part_ref[g, pl.ds(r, HEADS), :] = out
                stat[pl.ds(r, HEADS), :] = st
            for d in range(2):
                for copy in writes(b0 + d):
                    copy.start()
            return carry

        lax.fori_loop(0, OWN_E // 2, pair, 0)
        part_ref[g, pl.ds(OWN_E * HEADS, 8), pl.ds(0, OWN_E * HEADS)] = stat[...].T[0:8, :]
        return carry

    lax.fori_loop(0, RANKS, group, 0)
    for b in range(EARLY - 2 * LAG, EARLY):
        for copy in writes(b):
            copy.wait()


def late_kernel(pos_ref, q_ref, kv_ref, early_ref, wo_ref, k_ref, v_ref,
                out_ref, keep_k, keep_v,
                wobuf, key, stat, late, recv_e, recv_l, mixed, own,
                wsem, krs, vrs, es, er, ls, lr, gs, gr):
    me = lax.axis_index('sp')
    start = me * SLOTS

    def target(j):
        return lax.rem(me + j, RANKS)

    def sequence(n):
        return EARLY + target(n // OWN_L + 1) * OWN_L + lax.rem(n, OWN_L)

    def reads(n):
        b = sequence(n)
        return (pltpu.make_async_copy(k_ref.at[b], keep_k.at[n], krs.at[n]),
                pltpu.make_async_copy(v_ref.at[b], keep_v.at[n], vrs.at[n]))

    def wo_copy(c):
        return pltpu.make_async_copy(wo_ref.at[:, pl.ds(c * COLS, COLS)], wobuf.at[c], wsem.at[c])

    def remote(src, dst, send, recv, j):
        return pltpu.make_async_remote_copy(src_ref=src, dst_ref=dst, send_sem=send, recv_sem=recv,
                                            device_id={'sp': target(j)}, device_id_type=MESH)

    def early_copy(j):
        return remote(early_ref.at[target(j)], recv_e.at[RANKS - j], es.at[j], er.at[RANKS - j], j)

    def late_copy(j):
        return remote(late.at[j], recv_l.at[RANKS - j], ls.at[j], lr.at[RANKS - j], j)

    def start_reads(n, carry):
        for copy in reads(n):
            copy.start()
        return carry

    lax.fori_loop(0, LATE, start_reads, 0)
    for c in range(CHUNKS):
        wo_copy(c).start()

    barrier = pltpu.get_barrier_semaphore()
    for j in range(1, RANKS):
        pl.semaphore_signal(barrier, inc=1, device_id={'sp': target(j)}, device_id_type=MESH)
    pl.semaphore_wait(barrier, RANKS - 1)
    for j in range(1, RANKS):
        early_copy(j).start()
    recv_e[0] = early_ref[me]
    key[...] = head_columns()

    row16 = lax.broadcasted_iota(jnp.int32, (HEADS, 2 * KV), 0)
    col16 = lax.broadcasted_iota(jnp.int32, (HEADS, 2 * KV), 1)

    def attend(n):
        b = sequence(n)
        local = pos_ref[b] - start
        base = pl.ds(pl.multiple_of(b * HEADS, HEADS), HEADS)
        q = q_ref[base, :].astype(BF16)
        kv = kv_ref[base, :].astype(BF16)
        scores = scores_of(q, keep_k[n])
        live = key[...] < local * KV
        scores = jnp.where(live, scores, NEG_FILL)
        mine = jnp.where((local >= 0) & (local < SLOTS), row16 >> 1, 64)
        fresh = jnp.where(col16 == mine, scores_of(q, kv), NEG_FILL)
        fresh = jnp.max(fresh, axis=-1, keepdims=True)
        peak = jnp.maximum(jnp.max(scores, axis=-1, keepdims=True), fresh)
        e = jnp.where(live, jnp.exp(scores - peak), 0.0)
        ef = jnp.where(col16 == mine + KV, jnp.exp(fresh - peak), 0.0)
        total = jnp.sum(e, axis=-1, keepdims=True) + jnp.sum(ef, axis=-1, keepdims=True)
        out = jnp.dot(e.astype(BF16), keep_v[n], preferred_element_type=F32)
        out = out + jnp.dot(ef.astype(BF16), kv, preferred_element_type=F32)
        return out, stat_tile(peak, total)

    def group(g, carry):
        def pair(j, carry):
            n0 = g * OWN_L + 2 * j
            for d in range(2):
                for copy in reads(n0 + d):
                    copy.wait()
            for d in range(2):
                out, st = attend(n0 + d)
                r = pl.multiple_of((2 * j + d) * HEADS, HEADS)
                late[g + 1, pl.ds(r, HEADS), :] = out
                stat[pl.ds(r, HEADS), :] = st
            return carry

        lax.fori_loop(0, OWN_L // 2, pair, 0)
        late[g + 1, pl.ds(OWN_L * HEADS, 8), pl.ds(0, OWN_L * HEADS)] = stat[...].T[0:8, :]

        @pl.when(g + 1 < RANKS)
        def _():
            late_copy(g + 1).start()

        return carry

    lax.fori_loop(0, RANKS, group, 0)
    recv_l[0] = late[RANKS]

    def combine(recv, count):
        rows = count * HEADS
        stats = [recv[s, pl.ds(rows, 8), pl.ds(0, rows)].T for s in range(RANKS)]
        peak = stats[0][:, 0:1]
        for s in range(1, RANKS):
            peak = jnp.maximum(peak, stats[s][:, 0:1])
        total = jnp.zeros((rows, 1), F32)
        acc = jnp.zeros((rows, DIM), F32)
        for s in range(RANKS):
            w = jnp.exp(stats[s][:, 0:1] - peak)
            total = total + w * stats[s][:, 1:2]
            acc = acc + w * recv[s, pl.ds(0, rows), :]
        return acc / total

    for j in range(1, RANKS):
        early_copy(j).wait()
    mixed[pl.ds(0, OWN_E * HEADS), :] = combine(recv_e, OWN_E)
    for c in range(CHUNKS):
        wo_copy(c).wait()
    for j in range(1, RANKS):
        late_copy(j).wait()
    mixed[pl.ds(OWN_E * HEADS, OWN_L * HEADS), :] = combine(recv_l, OWN_L)
    attn = jnp.concatenate([mixed[pl.ds(h, OWN, stride=HEADS), :] for h in range(HEADS)], axis=1).astype(BF16)

    def gather_copy(c, j):
        block = pl.ds(c * COLS, COLS)
        return remote(own.at[:, block], out_ref.at[me, :, block], gs.at[c, j], gr.at[c, RANKS - j], j)

    for c in range(CHUNKS):
        own[:, pl.ds(c * COLS, COLS)] = jnp.dot(attn, wobuf[c], preferred_element_type=F32)
        for j in range(1, RANKS):
            gather_copy(c, j).start()
    out_ref[me] = own[...]
    for c in range(CHUNKS):
        for j in range(1, RANKS):
            gather_copy(c, j).wait()


def store_kernel(pos_ref, tok_ref, kv_ref, rows_ref, keep_k, keep_v, ko_in, vo_in,
                 out_ref, ko_ref, vo_ref, scr, fresh_k, fresh_v, kws, vws, fks, fvs):
    me = lax.axis_index('sp')
    start = me * SLOTS

    def sequence(n):
        return EARLY + lax.rem(me + n // OWN_L + 1, RANKS) * OWN_L + lax.rem(n, OWN_L)

    def writes(n):
        b = sequence(n)
        return (pltpu.make_async_copy(keep_k.at[n], ko_ref.at[b], kws.at[n]),
                pltpu.make_async_copy(keep_v.at[n], vo_ref.at[b], vws.at[n]))

    def fresh(n):
        b = sequence(n)
        local = pos_ref[b] - start
        block = pl.ds(pl.multiple_of(jnp.clip(local, 0, SLOTS - 1) * KV, KV), KV)
        return ((local >= 0) & (local < SLOTS),
                (pltpu.make_async_copy(fresh_k.at[n], ko_ref.at[b, block], fks), pltpu.make_async_copy(fresh_v.at[n], vo_ref.at[b, block], fvs)))

    def begin(n, carry):
        for copy in writes(n):
            copy.start()
        return carry

    lax.fori_loop(0, LATE, begin, 0)

    def stage(n, carry):
        base = pl.multiple_of(sequence(n) * 2 * KV, 2 * KV)
        fresh_k[n] = kv_ref[pl.ds(base, KV), :].astype(BF16)
        fresh_v[n] = kv_ref[pl.ds(pl.multiple_of(base + KV, KV), KV), :].astype(BF16)
        return carry

    lax.fori_loop(0, LATE, stage, 0)
    for d in range(RANKS):
        scr[pl.ds(d * OWN_E, OWN_E), :] = rows_ref[d, pl.ds(0, OWN_E), :]
        scr[pl.ds(EARLY + d * OWN_L, OWN_L), :] = rows_ref[d, pl.ds(OWN_E, OWN_L), :]
    out_ref[...] = (tok_ref[...].astype(F32) + scr[...]).astype(BF16)

    def follow(n, carry):
        mine, copies = fresh(n)
        for copy in writes(n):
            copy.wait()

        @pl.when(mine)
        def _():
            for copy in copies:
                copy.start()

        return carry

    lax.fori_loop(0, LATE, follow, 0)

    def drain(n, carry):
        mine, copies = fresh(n)

        @pl.when(mine)
        def _():
            for copy in copies:
                copy.wait()

        return carry

    lax.fori_loop(0, LATE, drain, 0)


def solution(mesh):
    cache_spec = P('dp', 'sp', None, None)
    hbm = pl.BlockSpec(memory_space=pltpu.HBM)
    vmem = pl.BlockSpec(memory_space=pltpu.VMEM)
    smem = pl.BlockSpec(memory_space=pltpu.SMEM)
    sds = jax.ShapeDtypeStruct
    flat = (SEQS, ROWS, DIM)
    dma = pltpu.SemaphoreType.DMA
    space = pltpu.VMEM

    def in_vmem(a):
        return pltpu.with_memory_space_constraint(a, pltpu.VMEM)

    def in_hbm(a):
        return pltpu.with_memory_space_constraint(a, pltpu.HBM)

    def device_step(tokens, positions, k_cache, v_cache, w_q, w_k, w_v, w_o, attn_norm, q_norm, k_norm):
        k_flat, v_flat = k_cache.reshape(flat), v_cache.reshape(flat)
        early, q, kv, new, k_out, v_out = pl.pallas_call(
            early_kernel,
            out_shape=(space((RANKS, PART_E, DIM), F32), space((SEQS * HEADS, DIM), F32), space((SEQS * 2 * KV, DIM), F32),
                       sds((SEQS * 2 * KV, DIM), BF16), sds(flat, BF16), sds(flat, BF16)),
            in_specs=[smem] + [vmem] * 5 + [hbm] * 5,
            out_specs=(vmem,) * 4 + (hbm,) * 2,
            scratch_shapes=[
                space((8, WIDTH, CHUNK), BF16), space((SEQS, WIDTH), BF16), space((SEQS, DIM), F32), space((SEQS, DIM), F32),
                space((HEADS, ROWS), jnp.int32), space((OWN_E * HEADS, DIM), F32),
                space((RING, ROWS, DIM), BF16), space((RING, ROWS, DIM), BF16),
                dma((8,)), dma((RING,)), dma((RING,)), dma((RING,)), dma((RING,)),
            ],
            compiler_params=pltpu.CompilerParams(vmem_limit_bytes=58 << 20),
        )(positions, tokens, frequencies(), attn_norm, q_norm, k_norm, in_hbm(w_q), in_hbm(w_k), in_hbm(w_v), in_hbm(k_flat), in_hbm(v_flat))
        rows, keep_k, keep_v = pl.pallas_call(
            late_kernel,
            out_shape=(space((RANKS, OWN, WIDTH), F32), space((LATE, ROWS, DIM), BF16), space((LATE, ROWS, DIM), BF16)),
            in_specs=[smem] + [vmem] * 3 + [hbm] * 3,
            out_specs=(vmem,) * 3,
            scratch_shapes=[
                space((CHUNKS, WIDTH, COLS), BF16), space((HEADS, ROWS), jnp.int32), space((OWN_L * HEADS, DIM), F32),
                space((RANKS + 1, PART_L, DIM), F32), space((RANKS, PART_E, DIM), F32), space((RANKS, PART_L, DIM), F32),
                space((OWN * HEADS, DIM), F32), space((OWN, WIDTH), F32),
                dma((CHUNKS,)), dma((LATE,)), dma((LATE,)), dma((RANKS,)), dma((RANKS,)), dma((RANKS,)), dma((RANKS,)),
                dma((CHUNKS, RANKS)), dma((CHUNKS, RANKS)),
            ],
            compiler_params=pltpu.CompilerParams(collective_id=0, has_side_effects=True, vmem_limit_bytes=12 << 20),
        )(positions, in_vmem(q), in_vmem(kv), in_vmem(early), in_hbm(w_o), in_hbm(k_flat), in_hbm(v_flat))
        block_out, k_out, v_out = pl.pallas_call(
            store_kernel,
            out_shape=(sds((SEQS, WIDTH), BF16), sds(flat, BF16), sds(flat, BF16)),
            in_specs=[smem] + [vmem] * 5 + [hbm] * 2,
            out_specs=(vmem, hbm, hbm),
            scratch_shapes=[space((SEQS, WIDTH), F32), space((LATE, KV, DIM), BF16), space((LATE, KV, DIM), BF16),
                            dma((LATE,)), dma((LATE,)), dma, dma],
            input_output_aliases={6: 1, 7: 2},
            compiler_params=pltpu.CompilerParams(vmem_limit_bytes=4 << 20),
        )(positions, tokens, in_vmem(kv), in_vmem(rows), in_vmem(keep_k), in_vmem(keep_v), k_out, v_out)
        return block_out, k_out.reshape(k_cache.shape), v_out.reshape(v_cache.shape), new.reshape(SEQS, 2, KV, DIM)

    return jax.shard_map(device_step, mesh=mesh, in_specs=(P('dp', None), P('dp'), cache_spec, cache_spec, P(), P(), P(), P(), P(), P(), P()), out_specs=(P('dp', None), cache_spec, cache_spec, P('dp', None, None, None)), check_vma=False)
```

```python
import jax
import jax.numpy as jnp
import numpy as np
from jax import lax
from jax.experimental import pallas as pl
from jax.experimental.pallas import tpu as pltpu
from jax.sharding import PartitionSpec as P

NORM_EPS = 1e-6
ROPE_THETA = 1000000.0
NEG_FILL = -1e30
F32 = jnp.float32
BF16 = jnp.bfloat16
MESH = pl.DeviceIdType.MESH

SEQS = 64
WIDTH = 2048
HEADS = 16
KV = 8
DIM = 128
SLOTS = 256
ROWS = SLOTS * KV
RANKS = 8
OWN = SEQS // RANKS
EARLY = 32
LATE = SEQS - EARLY
OWN_E = EARLY // RANKS
OWN_L = LATE // RANKS
PART_E = OWN_E * HEADS + 8
PART_L = OWN_L * HEADS + 8
CHUNK = 512
RING = 16
PAIRS = RING // 2
LAG = 3
AHEAD = 8
COLS = 512
CHUNKS = WIDTH // COLS


def frequencies():
    half = ROPE_THETA ** (-np.arange(DIM // 2, dtype=np.float64) * 2.0 / DIM)
    return jnp.asarray(np.concatenate([half, half])[None, :], F32)


def head_columns():
    row = lax.broadcasted_iota(jnp.int32, (HEADS, ROWS), 0)
    col = lax.broadcasted_iota(jnp.int32, (HEADS, ROWS), 1)
    return jnp.where((col & (KV - 1)) == (row >> 1), col, 1 << 30)


def insert(buf, index, local, new):
    row = lax.broadcasted_iota(jnp.int32, (2 * KV, DIM), 0)
    slot = jnp.clip(local, 0, SLOTS - 1)
    first = jnp.where(local == slot, (slot & 1) * KV, 64)
    block = pl.ds(pl.multiple_of((slot >> 1) * 2 * KV, 2 * KV), 2 * KV)
    both = jnp.concatenate([new, new], axis=0)
    old = buf[index, block, :].astype(F32)
    hit = (row >= first) & (row < first + KV)
    buf[index, block, :] = jnp.where(hit, both, old).astype(BF16)


def scores_of(q, k):
    return lax.dot_general(q, k, (((1,), (1,)), ((), ())), preferred_element_type=F32) * (DIM ** -0.5)


def stat_tile(peak, total):
    lane = lax.broadcasted_iota(jnp.int32, (HEADS, DIM), 1)
    return jnp.where(lane == 0, peak, total)


def early_kernel(pos_ref, tok_ref, freq_ref, an_ref, qn_ref, kn_ref, wq_ref, wk_ref, wv_ref, k_ref, v_ref,
                 part_ref, q_scr, kv_scr, new_ref, ko_ref, vo_ref,
                 wbuf, hid, cos_scr, sin_scr, key, stat, kbuf, vbuf, wsem, krs, vrs, kws, vws):
    start = lax.axis_index('sp') * SLOTS

    def weight_copy(c):
        if c < 4:
            src = wq_ref.at[:, pl.ds(c * CHUNK, CHUNK)]
        elif c < 6:
            src = wk_ref.at[:, pl.ds((c - 4) * CHUNK, CHUNK)]
        else:
            src = wv_ref.at[:, pl.ds((c - 6) * CHUNK, CHUNK)]
        return pltpu.make_async_copy(src, wbuf.at[c], wsem.at[c])

    def reads(b):
        s = lax.rem(b, RING)
        return (pltpu.make_async_copy(k_ref.at[b], kbuf.at[s], krs.at[s]),
                pltpu.make_async_copy(v_ref.at[b], vbuf.at[s], vrs.at[s]))

    def writes(b):
        s = lax.rem(b, RING)
        return (pltpu.make_async_copy(kbuf.at[s], ko_ref.at[b], kws.at[s]),
                pltpu.make_async_copy(vbuf.at[s], vo_ref.at[b], vws.at[s]))

    for c in range(8):
        weight_copy(c).start()

    def first_reads(b, carry):
        for copy in reads(b):
            copy.start()
        return carry

    lax.fori_loop(0, RING, first_reads, 0)

    x = tok_ref[...].astype(F32)
    scale = lax.rsqrt(jnp.mean(x * x, axis=-1, keepdims=True) + NORM_EPS)
    hid[...] = (x * scale * an_ref[...].astype(F32)[None, :]).astype(BF16)

    def fill(b, carry):
        cos_scr[pl.ds(b, 1), :] = jnp.full((1, DIM), pos_ref[b].astype(F32), F32)
        return carry

    lax.fori_loop(0, SEQS, fill, 0)
    angle = cos_scr[...] * freq_ref[...]
    lane = lax.broadcasted_iota(jnp.int32, (SEQS, DIM), 1)
    sin = jnp.sin(angle)
    cos_scr[...] = jnp.cos(angle)
    sin_scr[...] = jnp.where(lane < DIM // 2, -sin, sin)
    key[...] = head_columns()

    def norm_rope(y, gain):
        y = y * lax.rsqrt(jnp.mean(y * y, axis=-1, keepdims=True) + NORM_EPS) * gain
        return (y * cos_scr[...] + pltpu.roll(y, DIM // 2, 1) * sin_scr[...]).astype(BF16).astype(F32)

    qg = qn_ref[...].astype(F32)[None, :]
    kg = kn_ref[...].astype(F32)[None, :]
    for c in range(8):
        weight_copy(c).wait()
        y = jnp.dot(hid[...], wbuf[c], preferred_element_type=F32).astype(BF16).astype(F32)
        for j in range(CHUNK // DIM):
            yh = y[:, j * DIM:(j + 1) * DIM]
            if c < 4:
                q_scr[pl.ds(c * 4 + j, SEQS, stride=HEADS), :] = norm_rope(yh, qg)
            elif c < 6:
                kv_scr[pl.ds((c - 4) * 4 + j, SEQS, stride=2 * KV), :] = norm_rope(yh, kg)
            else:
                kv_scr[pl.ds(KV + (c - 6) * 4 + j, SEQS, stride=2 * KV), :] = yh
    new_ref[...] = kv_scr[...].astype(BF16)

    def attend(b):
        s = lax.rem(b, RING)
        local = pos_ref[b] - start
        q = q_scr[pl.ds(pl.multiple_of(b * HEADS, HEADS), HEADS), :].astype(BF16)
        scores = scores_of(q, kbuf[s])
        live = key[...] < (local + 1) * KV
        scores = jnp.where(live, scores, NEG_FILL)
        peak = jnp.max(scores, axis=-1, keepdims=True)
        e = jnp.where(live, jnp.exp(scores - peak), 0.0)
        total = jnp.sum(e, axis=-1, keepdims=True)
        out = jnp.dot(e.astype(BF16), vbuf[s], preferred_element_type=F32)
        return out, stat_tile(peak, total)

    def group(g, carry):
        def pair(j, carry):
            i = g * (OWN_E // 2) + j
            b0 = 2 * i

            @pl.when(i >= LAG)
            def _():
                for d in range(2):
                    for copy in writes(b0 - 2 * LAG + d):
                        copy.wait()

            @pl.when((i >= LAG) & (i - LAG + PAIRS < EARLY // 2))
            def _():
                for d in range(2):
                    for copy in reads(b0 - 2 * LAG + RING + d):
                        copy.start()

            for d in range(2):
                for copy in reads(b0 + d):
                    copy.wait()
            for d in range(2):
                b = b0 + d
                s = lax.rem(b, RING)
                local = pos_ref[b] - start
                base = pl.multiple_of(b * 2 * KV, 2 * KV)
                insert(kbuf, s, local, kv_scr[pl.ds(base, KV), :])
                insert(vbuf, s, local, kv_scr[pl.ds(pl.multiple_of(base + KV, KV), KV), :])
            for d in range(2):
                out, st = attend(b0 + d)
                r = pl.multiple_of((2 * j + d) * HEADS, HEADS)
                part_ref[g, pl.ds(r, HEADS), :] = out
                stat[pl.ds(r, HEADS), :] = st
            for d in range(2):
                for copy in writes(b0 + d):
                    copy.start()
            return carry

        lax.fori_loop(0, OWN_E // 2, pair, 0)
        part_ref[g, pl.ds(OWN_E * HEADS, 8), pl.ds(0, OWN_E * HEADS)] = stat[...].T[0:8, :]
        return carry

    lax.fori_loop(0, RANKS, group, 0)
    for b in range(EARLY - 2 * LAG, EARLY):
        for copy in writes(b):
            copy.wait()


def bit(value, place):
    if isinstance(value, int):
        return value // place % 2
    return lax.rem(lax.div(value, place), 2)


def flip(index, mask):
    return sum(lax.rem(bit(index, p) + bit(mask, p), 2) * p for p in (1, 2, 4))


def late_sequence(me, n):
    return EARLY + flip(me, RANKS - 1 - lax.div(n, OWN_L)) * OWN_L + lax.rem(n, OWN_L)


def late_kernel(pos_ref, q_ref, kv_ref, early_ref, wo_ref, k_ref, v_ref,
                out_e, out_l, keep_k, keep_v,
                wobuf, key, stat, late, recv_e, recv_l, mixed, own_e, own_l,
                wsem, krs, vrs, es, er, ls, lr, ges, ger, gls, glr):
    me = lax.axis_index('sp')
    start = me * SLOTS

    def reads(n):
        b = late_sequence(me, n)
        return (pltpu.make_async_copy(k_ref.at[b], keep_k.at[n], krs.at[n]),
                pltpu.make_async_copy(v_ref.at[b], keep_v.at[n], vrs.at[n]))

    def wo_copy(c):
        return pltpu.make_async_copy(wo_ref.at[:, pl.ds(pl.multiple_of(c * COLS, COLS), COLS)], wobuf.at[c], wsem.at[c])

    def remote(src, dst, send, recv, mask):
        return pltpu.make_async_remote_copy(src_ref=src, dst_ref=dst, send_sem=send, recv_sem=recv,
                                            device_id={'sp': flip(me, mask)}, device_id_type=MESH)

    def early_copy(m):
        return remote(early_ref.at[flip(me, m)], recv_e.at[m], es.at[m], er.at[m], m)

    def late_copy(m):
        return remote(late.at[m], recv_l.at[m], ls.at[m], lr.at[m], m)

    def start_reads(n, carry):
        for copy in reads(n):
            copy.start()
        return carry

    lax.fori_loop(0, AHEAD, start_reads, 0)

    barrier = pltpu.get_barrier_semaphore()
    for m in range(1, RANKS):
        pl.semaphore_signal(barrier, inc=1, device_id={'sp': flip(me, m)}, device_id_type=MESH)
    pl.semaphore_wait(barrier, RANKS - 1)
    for m in range(RANKS - 1, 0, -1):
        early_copy(m).start()
    recv_e[0] = early_ref[me]
    key[...] = head_columns()

    row16 = lax.broadcasted_iota(jnp.int32, (HEADS, 2 * KV), 0)
    col16 = lax.broadcasted_iota(jnp.int32, (HEADS, 2 * KV), 1)

    def attend(n):
        b = late_sequence(me, n)
        local = pos_ref[b] - start
        base = pl.ds(pl.multiple_of(b * HEADS, HEADS), HEADS)
        q = q_ref[base, :].astype(BF16)
        kv = kv_ref[base, :].astype(BF16)
        scores = scores_of(q, keep_k[n])
        live = key[...] < local * KV
        scores = jnp.where(live, scores, NEG_FILL)
        mine = jnp.where((local >= 0) & (local < SLOTS), row16 >> 1, 64)
        fresh = jnp.where(col16 == mine, scores_of(q, kv), NEG_FILL)
        fresh = jnp.max(fresh, axis=-1, keepdims=True)
        peak = jnp.maximum(jnp.max(scores, axis=-1, keepdims=True), fresh)
        e = jnp.where(live, jnp.exp(scores - peak), 0.0)
        ef = jnp.where(col16 == mine + KV, jnp.exp(fresh - peak), 0.0)
        total = jnp.sum(e, axis=-1, keepdims=True) + jnp.sum(ef, axis=-1, keepdims=True)
        out = jnp.dot(e.astype(BF16), keep_v[n], preferred_element_type=F32)
        out = out + jnp.dot(ef.astype(BF16), kv, preferred_element_type=F32)
        return out, stat_tile(peak, total)

    def group(g, carry):
        m = RANKS - 1 - g

        @pl.when(g < CHUNKS)
        def _():
            wo_copy(g).start()

        def pair(j, carry):
            n0 = g * OWN_L + 2 * j

            @pl.when(n0 + AHEAD < LATE)
            def _():
                for d in range(2):
                    start_reads(n0 + AHEAD + d, 0)

            for d in range(2):
                for copy in reads(n0 + d):
                    copy.wait()
            for d in range(2):
                out, st = attend(n0 + d)
                r = pl.multiple_of((2 * j + d) * HEADS, HEADS)
                late[m, pl.ds(r, HEADS), :] = out
                stat[pl.ds(r, HEADS), :] = st
            return carry

        lax.fori_loop(0, OWN_L // 2, pair, 0)
        late[m, pl.ds(OWN_L * HEADS, 8), pl.ds(0, OWN_L * HEADS)] = stat[...].T[0:8, :]

        @pl.when(g + 1 < RANKS)
        def _():
            late_copy(m).start()

        return carry

    def combine(recv, count):
        rows = count * HEADS
        stats = [recv[s, pl.ds(rows, 8), pl.ds(0, rows)].T for s in range(RANKS)]
        peak = stats[0][:, 0:1]
        for s in range(1, RANKS):
            peak = jnp.maximum(peak, stats[s][:, 0:1])
        total = jnp.zeros((rows, 1), F32)
        acc = jnp.zeros((rows, DIM), F32)
        for s in range(RANKS):
            w = jnp.exp(stats[s][:, 0:1] - peak)
            total = total + w * stats[s][:, 1:2]
            acc = acc + w * recv[s, pl.ds(0, rows), :]
        mixed[...] = acc / total
        return jnp.concatenate([mixed[pl.ds(h, count, stride=HEADS), :] for h in range(HEADS)], axis=1).astype(BF16)

    def gather(c, own, out, gs, gr):
        block = pl.ds(c * COLS, COLS)

        def send(mask):
            return remote(own.at[:, block], out.at[me, :, block], gs.at[c, mask], gr.at[c, me], mask)

        def relay(mask):
            src = flip(me, mask)
            return remote(out.at[src, :, block], out.at[src, :, block], gs.at[c, mask + 1], gr.at[c, src], 1)

        def arrival(mask):
            src = flip(me, mask)
            return remote(own.at[:, block], out.at[src, :, block], gs.at[c, mask], gr.at[c, src], mask)

        def first():
            for mask in (6, 4, 2, 1):
                send(mask).start()

        def second():
            for mask in (2, 4, 6):
                arrival(mask).wait_recv()
                relay(mask).start()

        def last():
            for mask in (1, 3, 5, 7):
                arrival(mask).wait_recv()
            for mask in (6, 4, 2, 1):
                send(mask).wait_send()
            for mask in (2, 4, 6):
                relay(mask).wait_send()

        return first, second, last

    def project(recv, count, own, out, gs, gr):
        attn = combine(recv, count)
        stages = [gather(c, own, out, gs, gr) for c in range(2)]
        for c in range(2):
            block = pl.ds(c * COLS, COLS)
            own[pl.ds(0, count), block] = jnp.dot(attn, wobuf[c], preferred_element_type=F32)
            own[pl.ds(count, count), block] = jnp.dot(attn, wobuf[c + 2], preferred_element_type=F32)
            stages[c][0]()
        out[me] = own[...]
        return stages

    lax.fori_loop(0, RANKS // 2, group, 0)
    for m in range(RANKS - 1, 0, -1):
        early_copy(m).wait()
    for c in range(CHUNKS):
        wo_copy(c).wait()
    stages_e = project(recv_e, OWN_E, own_e, out_e, ges, ger)
    lax.fori_loop(RANKS // 2, RANKS, group, 0)
    for stage in stages_e:
        stage[1]()
    recv_l[0] = late[0]
    for m in range(RANKS - 1, 0, -1):
        late_copy(m).wait()
    stages_l = project(recv_l, OWN_L, own_l, out_l, gls, glr)
    for stage in stages_l:
        stage[1]()
    for stage in stages_e + stages_l:
        stage[2]()


def store_kernel(pos_ref, tok_ref, kv_ref, rows_e, rows_l, keep_k, keep_v, ko_in, vo_in,
                 out_ref, ko_ref, vo_ref, scr, fresh_k, fresh_v, kws, vws, fks, fvs):
    me = lax.axis_index('sp')
    start = me * SLOTS

    def writes(n):
        b = late_sequence(me, n)
        return (pltpu.make_async_copy(keep_k.at[n], ko_ref.at[b], kws.at[n]),
                pltpu.make_async_copy(keep_v.at[n], vo_ref.at[b], vws.at[n]))

    def fresh(n):
        b = late_sequence(me, n)
        block = pl.ds(pl.multiple_of(jnp.clip(pos_ref[b] - start, 0, SLOTS - 1) * KV, KV), KV)
        return (pltpu.make_async_copy(fresh_k.at[n], ko_ref.at[b, block], fks), pltpu.make_async_copy(fresh_v.at[n], vo_ref.at[b, block], fvs))

    def each(action, wanted):
        def body(n, carry):
            local = pos_ref[late_sequence(me, n)] - start
            mine = (local >= 0) & (local < SLOTS)

            @pl.when(mine if wanted else jnp.logical_not(mine))
            def _():
                action(n)

            return carry

        lax.fori_loop(0, LATE, body, 0)

    def begin(n):
        for copy in writes(n):
            copy.start()

    def follow(n):
        for copy in writes(n):
            copy.wait()
        for copy in fresh(n):
            copy.start()

    def drain(n):
        for copy in writes(n):
            copy.wait()

    def drain_fresh(n):
        for copy in fresh(n):
            copy.wait()

    each(begin, True)
    each(begin, False)

    def stage(n, carry):
        base = pl.multiple_of(late_sequence(me, n) * 2 * KV, 2 * KV)
        fresh_k[n] = kv_ref[pl.ds(base, KV), :].astype(BF16)
        fresh_v[n] = kv_ref[pl.ds(pl.multiple_of(base + KV, KV), KV), :].astype(BF16)
        return carry

    lax.fori_loop(0, LATE, stage, 0)
    half = WIDTH // 2
    for rows, first, count in ((rows_e, 0, OWN_E), (rows_l, EARLY, OWN_L)):
        for d in range(RANKS):
            scr[pl.ds(first + d * count, count), pl.ds(0, half)] = rows[d, pl.ds(0, count), :]
            scr[pl.ds(first + d * count, count), pl.ds(half, half)] = rows[d, pl.ds(count, count), :]
    out_ref[...] = (tok_ref[...].astype(F32) + scr[...]).astype(BF16)
    each(follow, True)
    each(drain, False)
    each(drain_fresh, True)


def solution(mesh):
    cache_spec = P('dp', 'sp', None, None)
    hbm = pl.BlockSpec(memory_space=pltpu.HBM)
    vmem = pl.BlockSpec(memory_space=pltpu.VMEM)
    smem = pl.BlockSpec(memory_space=pltpu.SMEM)
    sds = jax.ShapeDtypeStruct
    flat = (SEQS, ROWS, DIM)
    dma = pltpu.SemaphoreType.DMA
    space = pltpu.VMEM

    def in_vmem(a):
        return pltpu.with_memory_space_constraint(a, pltpu.VMEM)

    def in_hbm(a):
        return pltpu.with_memory_space_constraint(a, pltpu.HBM)

    def device_step(tokens, positions, k_cache, v_cache, w_q, w_k, w_v, w_o, attn_norm, q_norm, k_norm):
        k_flat, v_flat = k_cache.reshape(flat), v_cache.reshape(flat)
        early, q, kv, new, k_out, v_out = pl.pallas_call(
            early_kernel,
            out_shape=(space((RANKS, PART_E, DIM), F32), space((SEQS * HEADS, DIM), F32), space((SEQS * 2 * KV, DIM), F32),
                       sds((SEQS * 2 * KV, DIM), BF16), sds(flat, BF16), sds(flat, BF16)),
            in_specs=[smem] + [vmem] * 5 + [hbm] * 5,
            out_specs=(vmem,) * 4 + (hbm,) * 2,
            scratch_shapes=[
                space((8, WIDTH, CHUNK), BF16), space((SEQS, WIDTH), BF16), space((SEQS, DIM), F32), space((SEQS, DIM), F32),
                space((HEADS, ROWS), jnp.int32), space((OWN_E * HEADS, DIM), F32),
                space((RING, ROWS, DIM), BF16), space((RING, ROWS, DIM), BF16),
                dma((8,)), dma((RING,)), dma((RING,)), dma((RING,)), dma((RING,)),
            ],
            compiler_params=pltpu.CompilerParams(vmem_limit_bytes=58 << 20),
        )(positions, tokens, frequencies(), attn_norm, q_norm, k_norm, in_hbm(w_q), in_hbm(w_k), in_hbm(w_v), in_hbm(k_flat), in_hbm(v_flat))
        rows_e, rows_l, keep_k, keep_v = pl.pallas_call(
            late_kernel,
            out_shape=(space((RANKS, 2 * OWN_E, WIDTH // 2), F32), space((RANKS, 2 * OWN_L, WIDTH // 2), F32),
                       space((LATE, ROWS, DIM), BF16), space((LATE, ROWS, DIM), BF16)),
            in_specs=[smem] + [vmem] * 3 + [hbm] * 3,
            out_specs=(vmem,) * 4,
            scratch_shapes=[
                space((CHUNKS, WIDTH, COLS), BF16), space((HEADS, ROWS), jnp.int32), space((OWN_L * HEADS, DIM), F32),
                space((RANKS, PART_L, DIM), F32), space((RANKS, PART_E, DIM), F32), space((RANKS, PART_L, DIM), F32),
                space((OWN_L * HEADS, DIM), F32), space((2 * OWN_E, WIDTH // 2), F32), space((2 * OWN_L, WIDTH // 2), F32),
                dma((CHUNKS,)), dma((LATE,)), dma((LATE,)), dma((RANKS,)), dma((RANKS,)), dma((RANKS,)), dma((RANKS,)),
                dma((2, RANKS)), dma((2, RANKS)), dma((2, RANKS)), dma((2, RANKS)),
            ],
            compiler_params=pltpu.CompilerParams(collective_id=0, has_side_effects=True, vmem_limit_bytes=12 << 20),
        )(positions, in_vmem(q), in_vmem(kv), in_vmem(early), in_hbm(w_o), in_hbm(k_flat), in_hbm(v_flat))
        block_out, k_out, v_out = pl.pallas_call(
            store_kernel,
            out_shape=(sds((SEQS, WIDTH), BF16), sds(flat, BF16), sds(flat, BF16)),
            in_specs=[smem] + [vmem] * 6 + [hbm] * 2,
            out_specs=(vmem, hbm, hbm),
            scratch_shapes=[space((SEQS, WIDTH), F32), space((LATE, KV, DIM), BF16), space((LATE, KV, DIM), BF16),
                            dma((LATE,)), dma((LATE,)), dma, dma],
            input_output_aliases={7: 1, 8: 2},
            compiler_params=pltpu.CompilerParams(vmem_limit_bytes=4 << 20),
        )(positions, tokens, in_vmem(kv), in_vmem(rows_e), in_vmem(rows_l), in_vmem(keep_k), in_vmem(keep_v), k_out, v_out)
        return block_out, k_out.reshape(k_cache.shape), v_out.reshape(v_cache.shape), new.reshape(SEQS, 2, KV, DIM)

    return jax.shard_map(device_step, mesh=mesh, in_specs=(P('dp', None), P('dp'), cache_spec, cache_spec, P(), P(), P(), P(), P(), P(), P()), out_specs=(P('dp', None), cache_spec, cache_spec, P('dp', None, None, None)), check_vma=False)
```

```python
import jax
import jax.numpy as jnp
import numpy as np
from jax import lax
from jax.experimental import pallas as pl
from jax.experimental.pallas import tpu as pltpu
from jax.sharding import PartitionSpec as P

NORM_EPS = 1e-6
ROPE_THETA = 1000000.0
NEG_FILL = -1e30
F32 = jnp.float32
BF16 = jnp.bfloat16
MESH = pl.DeviceIdType.MESH

SEQS = 64
WIDTH = 2048
HEADS = 16
KV = 8
DIM = 128
SLOTS = 256
ROWS = SLOTS * KV
RANKS = 8
OWN = SEQS // RANKS
EARLY = 32
LATE = SEQS - EARLY
OWN_E = EARLY // RANKS
OWN_L = LATE // RANKS
PART_E = OWN_E * HEADS + 8
PART_L = OWN_L * HEADS + 8
CHUNK = 512
RING = 16
PAIRS = RING // 2
LAG = 3
AHEAD = 8
COLS = 512
CHUNKS = WIDTH // COLS


def frequencies():
    half = ROPE_THETA ** (-np.arange(DIM // 2, dtype=np.float64) * 2.0 / DIM)
    return jnp.asarray(np.concatenate([half, half])[None, :], F32)


def head_columns():
    row = lax.broadcasted_iota(jnp.int32, (HEADS, ROWS), 0)
    col = lax.broadcasted_iota(jnp.int32, (HEADS, ROWS), 1)
    return jnp.where((col & (KV - 1)) == (row >> 1), col, 1 << 30)


def insert(buf, index, local, new):
    row = lax.broadcasted_iota(jnp.int32, (2 * KV, DIM), 0)
    slot = jnp.clip(local, 0, SLOTS - 1)
    first = jnp.where(local == slot, (slot & 1) * KV, 64)
    block = pl.ds(pl.multiple_of((slot >> 1) * 2 * KV, 2 * KV), 2 * KV)
    both = jnp.concatenate([new, new], axis=0)
    old = buf[index, block, :].astype(F32)
    hit = (row >= first) & (row < first + KV)
    buf[index, block, :] = jnp.where(hit, both, old).astype(BF16)


def scores_of(q, k):
    return lax.dot_general(q, k, (((1,), (1,)), ((), ())), preferred_element_type=F32) * (DIM ** -0.5)


def stat_tile(peak, total):
    lane = lax.broadcasted_iota(jnp.int32, (HEADS, DIM), 1)
    return jnp.where(lane == 0, peak, total)


def early_kernel(pos_ref, tok_ref, freq_ref, an_ref, qn_ref, kn_ref, wq_ref, wk_ref, wv_ref, k_ref, v_ref,
                 part_ref, q_scr, kv_scr, new_ref, ko_ref, vo_ref,
                 wbuf, hid, cos_scr, sin_scr, key, stat, kbuf, vbuf, wsem, krs, vrs, kws, vws):
    start = lax.axis_index('sp') * SLOTS

    def weight_copy(c):
        if c < 4:
            src = wq_ref.at[:, pl.ds(c * CHUNK, CHUNK)]
        elif c < 6:
            src = wk_ref.at[:, pl.ds((c - 4) * CHUNK, CHUNK)]
        else:
            src = wv_ref.at[:, pl.ds((c - 6) * CHUNK, CHUNK)]
        return pltpu.make_async_copy(src, wbuf.at[c], wsem.at[c])

    def reads(b):
        s = lax.rem(b, RING)
        return (pltpu.make_async_copy(k_ref.at[b], kbuf.at[s], krs.at[s]),
                pltpu.make_async_copy(v_ref.at[b], vbuf.at[s], vrs.at[s]))

    def writes(b):
        s = lax.rem(b, RING)
        return (pltpu.make_async_copy(kbuf.at[s], ko_ref.at[b], kws.at[s]),
                pltpu.make_async_copy(vbuf.at[s], vo_ref.at[b], vws.at[s]))

    for c in range(8):
        weight_copy(c).start()

    def first_reads(b, carry):
        for copy in reads(b):
            copy.start()
        return carry

    lax.fori_loop(0, RING, first_reads, 0)

    x = tok_ref[...].astype(F32)
    scale = lax.rsqrt(jnp.mean(x * x, axis=-1, keepdims=True) + NORM_EPS)
    hid[...] = (x * scale * an_ref[...].astype(F32)[None, :]).astype(BF16)

    def fill(b, carry):
        cos_scr[pl.ds(b, 1), :] = jnp.full((1, DIM), pos_ref[b].astype(F32), F32)
        return carry

    lax.fori_loop(0, SEQS, fill, 0)
    angle = cos_scr[...] * freq_ref[...]
    lane = lax.broadcasted_iota(jnp.int32, (SEQS, DIM), 1)
    sin = jnp.sin(angle)
    cos_scr[...] = jnp.cos(angle)
    sin_scr[...] = jnp.where(lane < DIM // 2, -sin, sin)
    key[...] = head_columns()

    def norm_rope(y, gain):
        y = y * lax.rsqrt(jnp.mean(y * y, axis=-1, keepdims=True) + NORM_EPS) * gain
        return (y * cos_scr[...] + pltpu.roll(y, DIM // 2, 1) * sin_scr[...]).astype(BF16).astype(F32)

    qg = qn_ref[...].astype(F32)[None, :]
    kg = kn_ref[...].astype(F32)[None, :]
    for c in range(8):
        weight_copy(c).wait()
        y = jnp.dot(hid[...], wbuf[c], preferred_element_type=F32).astype(BF16).astype(F32)
        for j in range(CHUNK // DIM):
            yh = y[:, j * DIM:(j + 1) * DIM]
            if c < 4:
                q_scr[pl.ds(c * 4 + j, SEQS, stride=HEADS), :] = norm_rope(yh, qg)
            elif c < 6:
                kv_scr[pl.ds((c - 4) * 4 + j, SEQS, stride=2 * KV), :] = norm_rope(yh, kg)
            else:
                kv_scr[pl.ds(KV + (c - 6) * 4 + j, SEQS, stride=2 * KV), :] = yh
    new_ref[...] = kv_scr[...].astype(BF16)

    def attend(b):
        s = lax.rem(b, RING)
        local = pos_ref[b] - start
        q = q_scr[pl.ds(pl.multiple_of(b * HEADS, HEADS), HEADS), :].astype(BF16)
        scores = scores_of(q, kbuf[s])
        live = key[...] < (local + 1) * KV
        scores = jnp.where(live, scores, NEG_FILL)
        peak = jnp.max(scores, axis=-1, keepdims=True)
        e = jnp.where(live, jnp.exp(scores - peak), 0.0)
        total = jnp.sum(e, axis=-1, keepdims=True)
        out = jnp.dot(e.astype(BF16), vbuf[s], preferred_element_type=F32)
        return out, stat_tile(peak, total)

    def group(g, carry):
        def pair(j, carry):
            i = g * (OWN_E // 2) + j
            b0 = 2 * i

            @pl.when(i >= LAG)
            def _():
                for d in range(2):
                    for copy in writes(b0 - 2 * LAG + d):
                        copy.wait()

            @pl.when((i >= LAG) & (i - LAG + PAIRS < EARLY // 2))
            def _():
                for d in range(2):
                    for copy in reads(b0 - 2 * LAG + RING + d):
                        copy.start()

            for d in range(2):
                for copy in reads(b0 + d):
                    copy.wait()
            for d in range(2):
                b = b0 + d
                s = lax.rem(b, RING)
                local = pos_ref[b] - start
                base = pl.multiple_of(b * 2 * KV, 2 * KV)
                insert(kbuf, s, local, kv_scr[pl.ds(base, KV), :])
                insert(vbuf, s, local, kv_scr[pl.ds(pl.multiple_of(base + KV, KV), KV), :])
            for d in range(2):
                out, st = attend(b0 + d)
                r = pl.multiple_of((2 * j + d) * HEADS, HEADS)
                part_ref[g, pl.ds(r, HEADS), :] = out
                stat[pl.ds(r, HEADS), :] = st
            for d in range(2):
                for copy in writes(b0 + d):
                    copy.start()
            return carry

        lax.fori_loop(0, OWN_E // 2, pair, 0)
        part_ref[g, pl.ds(OWN_E * HEADS, 8), pl.ds(0, OWN_E * HEADS)] = stat[...].T[0:8, :]
        return carry

    lax.fori_loop(0, RANKS, group, 0)
    for b in range(EARLY - 2 * LAG, EARLY):
        for copy in writes(b):
            copy.wait()


def bit(value, place):
    if isinstance(value, int):
        return value // place % 2
    return lax.rem(lax.div(value, place), 2)


def flip(index, mask):
    return sum(lax.rem(bit(index, p) + bit(mask, p), 2) * p for p in (1, 2, 4))


def late_sequence(me, n):
    return EARLY + flip(me, RANKS - 1 - lax.div(n, OWN_L)) * OWN_L + lax.rem(n, OWN_L)


def late_kernel(pos_ref, q_ref, kv_ref, early_ref, wo_ref, k_ref, v_ref,
                out_e, out_l, wobuf, keep_k, keep_v,
                key, stat, late, recv_e, recv_l, own_e, own_l,
                wsem, krs, vrs, es, er, ls, lr, ges, ger, gls, glr):
    me = lax.axis_index('sp')
    start = me * SLOTS

    def reads(n):
        b = late_sequence(me, n)
        return (pltpu.make_async_copy(k_ref.at[b], keep_k.at[n], krs.at[n]),
                pltpu.make_async_copy(v_ref.at[b], keep_v.at[n], vrs.at[n]))

    def wo_copy(c):
        return pltpu.make_async_copy(wo_ref.at[:, pl.ds(pl.multiple_of(c * COLS, COLS), COLS)], wobuf.at[c], wsem.at[c])

    def remote(src, dst, send, recv, mask):
        return pltpu.make_async_remote_copy(src_ref=src, dst_ref=dst, send_sem=send, recv_sem=recv,
                                            device_id={'sp': flip(me, mask)}, device_id_type=MESH)

    def early_copy(m):
        return remote(early_ref.at[flip(me, m)], recv_e.at[m], es.at[m], er.at[m], m)

    def late_copy(m):
        return remote(late.at[m], recv_l.at[m], ls.at[m], lr.at[m], m)

    def start_reads(n, carry):
        for copy in reads(n):
            copy.start()
        return carry

    lax.fori_loop(0, 4, start_reads, 0)

    barrier = pltpu.get_barrier_semaphore()
    for m in range(1, RANKS):
        pl.semaphore_signal(barrier, inc=1, device_id={'sp': flip(me, m)}, device_id_type=MESH)
    pl.semaphore_wait(barrier, RANKS - 1)
    for m in range(RANKS - 1, 0, -1):
        early_copy(m).start()
    lax.fori_loop(4, AHEAD, start_reads, 0)
    recv_e[0] = early_ref[me]
    key[...] = head_columns()

    row16 = lax.broadcasted_iota(jnp.int32, (HEADS, 2 * KV), 0)
    col16 = lax.broadcasted_iota(jnp.int32, (HEADS, 2 * KV), 1)

    def attend(n):
        b = late_sequence(me, n)
        local = pos_ref[b] - start
        base = pl.ds(pl.multiple_of(b * HEADS, HEADS), HEADS)
        q = q_ref[base, :].astype(BF16)
        kv = kv_ref[base, :].astype(BF16)
        scores = scores_of(q, keep_k[n])
        live = key[...] < local * KV
        scores = jnp.where(live, scores, NEG_FILL)
        mine = jnp.where((local >= 0) & (local < SLOTS), row16 >> 1, 64)
        fresh = jnp.where(col16 == mine, scores_of(q, kv), NEG_FILL)
        fresh = jnp.max(fresh, axis=-1, keepdims=True)
        peak = jnp.maximum(jnp.max(scores, axis=-1, keepdims=True), fresh)
        e = jnp.where(live, jnp.exp(scores - peak), 0.0)
        ef = jnp.where(col16 == mine + KV, jnp.exp(fresh - peak), 0.0)
        total = jnp.sum(e, axis=-1, keepdims=True) + jnp.sum(ef, axis=-1, keepdims=True)
        out = jnp.dot(e.astype(BF16), keep_v[n], preferred_element_type=F32)
        out = out + jnp.dot(ef.astype(BF16), kv, preferred_element_type=F32)
        return out, stat_tile(peak, total)

    def group(g, carry):
        m = RANKS - 1 - g

        def pair(j, carry):
            n0 = g * OWN_L + 2 * j

            @pl.when(n0 + AHEAD < LATE)
            def _():
                for d in range(2):
                    start_reads(n0 + AHEAD + d, 0)

            @pl.when(n0 + AHEAD == LATE)
            def _():
                for c in range(CHUNKS):
                    wo_copy(c).start()

            for d in range(2):
                for copy in reads(n0 + d):
                    copy.wait()
            for d in range(2):
                out, st = attend(n0 + d)
                r = pl.multiple_of((2 * j + d) * HEADS, HEADS)
                late[m, pl.ds(r, HEADS), :] = out
                stat[pl.ds(r, HEADS), :] = st
            return carry

        lax.fori_loop(0, OWN_L // 2, pair, 0)
        late[m, pl.ds(OWN_L * HEADS, 8), pl.ds(0, OWN_L * HEADS)] = stat[...].T[0:8, :]

        @pl.when(g + 1 < RANKS)
        def _():
            late_copy(m).start()

        return carry

    def combine(recv, count):
        rows = count * HEADS
        stats = [recv[s, pl.ds(rows, 8), pl.ds(0, rows)].T for s in range(RANKS)]
        peak = stats[0][:, 0:1]
        for s in range(1, RANKS):
            peak = jnp.maximum(peak, stats[s][:, 0:1])
        total = jnp.zeros((rows, 1), F32)
        acc = jnp.zeros((rows, DIM), F32)
        for s in range(RANKS):
            w = jnp.exp(stats[s][:, 0:1] - peak)
            total = total + w * stats[s][:, 1:2]
            acc = acc + w * recv[s, pl.ds(0, rows), :]
        return acc / total

    def gather(own, out, gs, gr):
        size = own.shape[0]

        def place(rank):
            return out.at[pl.ds(pl.multiple_of(rank * size, size), size), :]

        def send(mask):
            return remote(own, place(me), gs.at[mask], gr.at[me], mask)

        def relay(mask):
            src = flip(me, mask)
            return remote(place(src), place(src), gs.at[mask + 1], gr.at[src], 1)

        def arrival(mask):
            src = flip(me, mask)
            return remote(own, place(src), gs.at[mask], gr.at[src], mask)

        def first():
            for mask in (6, 4, 2, 1):
                send(mask).start()
            out[pl.ds(pl.multiple_of(me * size, size), size), :] = own[...]

        def second():
            for mask in (2, 4, 6):
                arrival(mask).wait_recv()
                relay(mask).start()

        def last():
            for mask in (1, 3, 5, 7):
                arrival(mask).wait_recv()
            for mask in (6, 4, 2, 1):
                send(mask).wait_send()
            for mask in (2, 4, 6):
                relay(mask).wait_send()

        return first, second, last

    stages_e = gather(own_e, out_e, ges, ger)
    stages_l = gather(own_l, out_l, gls, glr)
    lax.fori_loop(0, RANKS - 1, group, 0)
    for m in range(RANKS - 1, 0, -1):
        early_copy(m).wait()
    own_e[...] = combine(recv_e, OWN_E)
    stages_e[0]()
    lax.fori_loop(RANKS - 1, RANKS, group, 0)
    recv_l[0] = late[0]
    for m in range(RANKS - 1, 0, -1):
        late_copy(m).wait()
    own_l[...] = combine(recv_l, OWN_L)
    stages_l[0]()
    stages_e[1]()
    stages_l[1]()
    for c in range(CHUNKS):
        wo_copy(c).wait()
    stages_e[2]()
    stages_l[2]()


def store_kernel(pos_ref, tok_ref, kv_ref, rows_e, rows_l, wobuf, keep_k_in, keep_v_in, ko_in, vo_in,
                 out_ref, keep_k, keep_v, ko_ref, vo_ref, attn, kws, vws):
    me = lax.axis_index('sp')
    start = me * SLOTS

    def writes(n):
        b = late_sequence(me, n)
        return (pltpu.make_async_copy(keep_k.at[n], ko_ref.at[b], kws), pltpu.make_async_copy(keep_v.at[n], vo_ref.at[b], vws))

    def step(n, carry):
        b = late_sequence(me, jnp.minimum(n, LATE - 1))
        local = pos_ref[b] - start

        @pl.when((n < LATE) & (local >= 0) & (local < SLOTS))
        def _():
            base = pl.multiple_of(b * 2 * KV, 2 * KV)
            insert(keep_k, n, local, kv_ref[pl.ds(base, KV), :])
            insert(keep_v, n, local, kv_ref[pl.ds(pl.multiple_of(base + KV, KV), KV), :])

        @pl.when(n >= 2)
        def _():
            for copy in writes(n - 2):
                copy.start()

        return carry

    lax.fori_loop(0, LATE + 2, step, 0)
    for h in range(HEADS):
        block = pl.ds(h * DIM, DIM)
        attn[pl.ds(0, EARLY), block] = rows_e[pl.ds(h, EARLY, stride=HEADS), :].astype(BF16)
        attn[pl.ds(EARLY, LATE), block] = rows_l[pl.ds(h, LATE, stride=HEADS), :].astype(BF16)
    for c in range(CHUNKS):
        block = pl.ds(c * COLS, COLS)
        y = jnp.dot(attn[...], wobuf[c], preferred_element_type=F32)
        out_ref[:, block] = (tok_ref[:, block].astype(F32) + y).astype(BF16)

    def drain(n, carry):
        for copy in writes(n):
            copy.wait()
        return carry

    lax.fori_loop(0, LATE, drain, 0)


def solution(mesh):
    cache_spec = P('dp', 'sp', None, None)
    hbm = pl.BlockSpec(memory_space=pltpu.HBM)
    vmem = pl.BlockSpec(memory_space=pltpu.VMEM)
    smem = pl.BlockSpec(memory_space=pltpu.SMEM)
    sds = jax.ShapeDtypeStruct
    flat = (SEQS, ROWS, DIM)
    dma = pltpu.SemaphoreType.DMA
    space = pltpu.VMEM

    def in_vmem(a):
        return pltpu.with_memory_space_constraint(a, pltpu.VMEM)

    def in_hbm(a):
        return pltpu.with_memory_space_constraint(a, pltpu.HBM)

    def device_step(tokens, positions, k_cache, v_cache, w_q, w_k, w_v, w_o, attn_norm, q_norm, k_norm):
        k_flat, v_flat = k_cache.reshape(flat), v_cache.reshape(flat)
        early, q, kv, new, k_out, v_out = pl.pallas_call(
            early_kernel,
            out_shape=(space((RANKS, PART_E, DIM), F32), space((SEQS * HEADS, DIM), F32), space((SEQS * 2 * KV, DIM), F32),
                       sds((SEQS * 2 * KV, DIM), BF16), sds(flat, BF16), sds(flat, BF16)),
            in_specs=[smem] + [vmem] * 5 + [hbm] * 5,
            out_specs=(vmem,) * 4 + (hbm,) * 2,
            scratch_shapes=[
                space((8, WIDTH, CHUNK), BF16), space((SEQS, WIDTH), BF16), space((SEQS, DIM), F32), space((SEQS, DIM), F32),
                space((HEADS, ROWS), jnp.int32), space((OWN_E * HEADS, DIM), F32),
                space((RING, ROWS, DIM), BF16), space((RING, ROWS, DIM), BF16),
                dma((8,)), dma((RING,)), dma((RING,)), dma((RING,)), dma((RING,)),
            ],
            compiler_params=pltpu.CompilerParams(vmem_limit_bytes=58 << 20),
        )(positions, tokens, frequencies(), attn_norm, q_norm, k_norm, in_hbm(w_q), in_hbm(w_k), in_hbm(w_v), in_hbm(k_flat), in_hbm(v_flat))
        rows_e, rows_l, wobuf, keep_k, keep_v = pl.pallas_call(
            late_kernel,
            out_shape=(space((EARLY * HEADS, DIM), F32), space((LATE * HEADS, DIM), F32), space((CHUNKS, WIDTH, COLS), BF16),
                       space((LATE, ROWS, DIM), BF16), space((LATE, ROWS, DIM), BF16)),
            in_specs=[smem] + [vmem] * 3 + [hbm] * 3,
            out_specs=(vmem,) * 5,
            scratch_shapes=[
                space((HEADS, ROWS), jnp.int32), space((OWN_L * HEADS, DIM), F32),
                space((RANKS, PART_L, DIM), F32), space((RANKS, PART_E, DIM), F32), space((RANKS, PART_L, DIM), F32),
                space((OWN_E * HEADS, DIM), F32), space((OWN_L * HEADS, DIM), F32),
                dma((CHUNKS,)), dma((LATE,)), dma((LATE,)), dma((RANKS,)), dma((RANKS,)), dma((RANKS,)), dma((RANKS,)),
                dma((RANKS,)), dma((RANKS,)), dma((RANKS,)), dma((RANKS,)),
            ],
            compiler_params=pltpu.CompilerParams(collective_id=0, has_side_effects=True, vmem_limit_bytes=3 << 20),
        )(positions, in_vmem(q), in_vmem(kv), in_vmem(early), in_hbm(w_o), in_hbm(k_flat), in_hbm(v_flat))
        block_out, _, _, k_out, v_out = pl.pallas_call(
            store_kernel,
            out_shape=(sds((SEQS, WIDTH), BF16), space((LATE, ROWS, DIM), BF16), space((LATE, ROWS, DIM), BF16), sds(flat, BF16), sds(flat, BF16)),
            in_specs=[smem] + [vmem] * 7 + [hbm] * 2,
            out_specs=(vmem, vmem, vmem, hbm, hbm),
            scratch_shapes=[space((SEQS, WIDTH), BF16), dma, dma],
            input_output_aliases={6: 1, 7: 2, 8: 3, 9: 4},
            compiler_params=pltpu.CompilerParams(vmem_limit_bytes=3 << 20),
        )(positions, tokens, in_vmem(kv), in_vmem(rows_e), in_vmem(rows_l), in_vmem(wobuf), in_vmem(keep_k), in_vmem(keep_v), k_out, v_out)
        return block_out, k_out.reshape(k_cache.shape), v_out.reshape(v_cache.shape), new.reshape(SEQS, 2, KV, DIM)

    return jax.shard_map(device_step, mesh=mesh, in_specs=(P('dp', None), P('dp'), cache_spec, cache_spec, P(), P(), P(), P(), P(), P(), P()), out_specs=(P('dp', None), cache_spec, cache_spec, P('dp', None, None, None)), check_vma=False)
```

```python
import jax
import jax.numpy as jnp
import numpy as np
from jax import lax
from jax.experimental import pallas as pl
from jax.experimental.pallas import tpu as pltpu
from jax.sharding import PartitionSpec as P

NORM_EPS = 1e-6
ROPE_THETA = 1000000.0
NEG_FILL = -1e30
F32 = jnp.float32
BF16 = jnp.bfloat16
MESH = pl.DeviceIdType.MESH

SEQS = 64
WIDTH = 2048
HEADS = 16
KV = 8
DIM = 128
SLOTS = 256
ROWS = SLOTS * KV
RANKS = 8
OWN = SEQS // RANKS
EARLY = 48
LATE = SEQS - EARLY
OWN_E = EARLY // RANKS
OWN_L = LATE // RANKS
PART_E = OWN_E * HEADS + 8
PART_L = OWN_L * HEADS + 8
CHUNK = 512
RING = 16
PAIRS = RING // 2
LAG = 3
AHEAD = 8
COLS = 512
CHUNKS = WIDTH // COLS


def frequencies():
    half = ROPE_THETA ** (-np.arange(DIM // 2, dtype=np.float64) * 2.0 / DIM)
    return jnp.asarray(np.concatenate([half, half])[None, :], F32)


def head_columns():
    row = lax.broadcasted_iota(jnp.int32, (HEADS, ROWS), 0)
    col = lax.broadcasted_iota(jnp.int32, (HEADS, ROWS), 1)
    return jnp.where((col & (KV - 1)) == (row >> 1), col, 1 << 30)


def insert(buf, index, local, new):
    row = lax.broadcasted_iota(jnp.int32, (2 * KV, DIM), 0)
    slot = jnp.clip(local, 0, SLOTS - 1)
    first = jnp.where(local == slot, (slot & 1) * KV, 64)
    block = pl.ds(pl.multiple_of((slot >> 1) * 2 * KV, 2 * KV), 2 * KV)
    both = jnp.concatenate([new, new], axis=0)
    old = buf[index, block, :].astype(F32)
    hit = (row >= first) & (row < first + KV)
    buf[index, block, :] = jnp.where(hit, both, old).astype(BF16)


def scores_of(q, k):
    return lax.dot_general(q, k, (((1,), (1,)), ((), ())), preferred_element_type=F32) * (DIM ** -0.5)


def stat_tile(peak, total):
    lane = lax.broadcasted_iota(jnp.int32, (HEADS, DIM), 1)
    return jnp.where(lane == 0, peak, total)


def early_kernel(pos_ref, tok_ref, freq_ref, an_ref, qn_ref, kn_ref, wq_ref, wk_ref, wv_ref, k_ref, v_ref,
                 part_ref, q_scr, kv_scr, new_ref, ko_ref, vo_ref,
                 wbuf, hid, cos_scr, sin_scr, key, stat, kbuf, vbuf, wsem, krs, vrs, kws, vws):
    start = lax.axis_index('sp') * SLOTS

    def weight_copy(c):
        if c < 4:
            src = wq_ref.at[:, pl.ds(c * CHUNK, CHUNK)]
        elif c < 6:
            src = wk_ref.at[:, pl.ds((c - 4) * CHUNK, CHUNK)]
        else:
            src = wv_ref.at[:, pl.ds((c - 6) * CHUNK, CHUNK)]
        return pltpu.make_async_copy(src, wbuf.at[c], wsem.at[c])

    def reads(b):
        s = lax.rem(b, RING)
        return (pltpu.make_async_copy(k_ref.at[b], kbuf.at[s], krs.at[s]),
                pltpu.make_async_copy(v_ref.at[b], vbuf.at[s], vrs.at[s]))

    def writes(b):
        s = lax.rem(b, RING)
        return (pltpu.make_async_copy(kbuf.at[s], ko_ref.at[b], kws.at[s]),
                pltpu.make_async_copy(vbuf.at[s], vo_ref.at[b], vws.at[s]))

    for c in range(8):
        weight_copy(c).start()

    def first_reads(b, carry):
        for copy in reads(b):
            copy.start()
        return carry

    lax.fori_loop(0, RING, first_reads, 0)

    x = tok_ref[...].astype(F32)
    scale = lax.rsqrt(jnp.mean(x * x, axis=-1, keepdims=True) + NORM_EPS)
    hid[...] = (x * scale * an_ref[...].astype(F32)[None, :]).astype(BF16)

    def fill(b, carry):
        cos_scr[pl.ds(b, 1), :] = jnp.full((1, DIM), pos_ref[b].astype(F32), F32)
        return carry

    lax.fori_loop(0, SEQS, fill, 0)
    angle = cos_scr[...] * freq_ref[...]
    lane = lax.broadcasted_iota(jnp.int32, (SEQS, DIM), 1)
    sin = jnp.sin(angle)
    cos_scr[...] = jnp.cos(angle)
    sin_scr[...] = jnp.where(lane < DIM // 2, -sin, sin)
    key[...] = head_columns()

    def norm_rope(y, gain):
        y = y * lax.rsqrt(jnp.mean(y * y, axis=-1, keepdims=True) + NORM_EPS) * gain
        return (y * cos_scr[...] + pltpu.roll(y, DIM // 2, 1) * sin_scr[...]).astype(BF16).astype(F32)

    qg = qn_ref[...].astype(F32)[None, :]
    kg = kn_ref[...].astype(F32)[None, :]
    for c in range(8):
        weight_copy(c).wait()
        y = jnp.dot(hid[...], wbuf[c], preferred_element_type=F32).astype(BF16).astype(F32)
        for j in range(CHUNK // DIM):
            yh = y[:, j * DIM:(j + 1) * DIM]
            if c < 4:
                q_scr[pl.ds(c * 4 + j, SEQS, stride=HEADS), :] = norm_rope(yh, qg)
            elif c < 6:
                kv_scr[pl.ds((c - 4) * 4 + j, SEQS, stride=2 * KV), :] = norm_rope(yh, kg)
            else:
                kv_scr[pl.ds(KV + (c - 6) * 4 + j, SEQS, stride=2 * KV), :] = yh
    new_ref[...] = kv_scr[...].astype(BF16)

    def attend(b):
        s = lax.rem(b, RING)
        local = pos_ref[b] - start
        q = q_scr[pl.ds(pl.multiple_of(b * HEADS, HEADS), HEADS), :].astype(BF16)
        scores = scores_of(q, kbuf[s])
        live = key[...] < (local + 1) * KV
        scores = jnp.where(live, scores, NEG_FILL)
        peak = jnp.max(scores, axis=-1, keepdims=True)
        e = jnp.where(live, jnp.exp(scores - peak), 0.0)
        total = jnp.sum(e, axis=-1, keepdims=True)
        out = jnp.dot(e.astype(BF16), vbuf[s], preferred_element_type=F32)
        return out, stat_tile(peak, total)

    def group(g, carry):
        def pair(j, carry):
            i = g * (OWN_E // 2) + j
            b0 = 2 * i

            @pl.when(i >= LAG)
            def _():
                for d in range(2):
                    for copy in writes(b0 - 2 * LAG + d):
                        copy.wait()

            @pl.when((i >= LAG) & (i - LAG + PAIRS < EARLY // 2))
            def _():
                for d in range(2):
                    for copy in reads(b0 - 2 * LAG + RING + d):
                        copy.start()

            for d in range(2):
                for copy in reads(b0 + d):
                    copy.wait()
            for d in range(2):
                b = b0 + d
                s = lax.rem(b, RING)
                local = pos_ref[b] - start
                base = pl.multiple_of(b * 2 * KV, 2 * KV)
                insert(kbuf, s, local, kv_scr[pl.ds(base, KV), :])
                insert(vbuf, s, local, kv_scr[pl.ds(pl.multiple_of(base + KV, KV), KV), :])
            for d in range(2):
                out, st = attend(b0 + d)
                r = pl.multiple_of((2 * j + d) * HEADS, HEADS)
                part_ref[g, pl.ds(r, HEADS), :] = out
                stat[pl.ds(r, HEADS), :] = st
            for d in range(2):
                for copy in writes(b0 + d):
                    copy.start()
            return carry

        lax.fori_loop(0, OWN_E // 2, pair, 0)
        part_ref[g, pl.ds(OWN_E * HEADS, 8), pl.ds(0, OWN_E * HEADS)] = stat[...].T[0:8, :]
        return carry

    lax.fori_loop(0, RANKS, group, 0)
    for b in range(EARLY - 2 * LAG, EARLY):
        for copy in writes(b):
            copy.wait()


def bit(value, place):
    if isinstance(value, int):
        return value // place % 2
    return lax.rem(lax.div(value, place), 2)


def flip(index, mask):
    return sum(lax.rem(bit(index, p) + bit(mask, p), 2) * p for p in (1, 2, 4))


def late_sequence(me, n):
    return EARLY + flip(me, RANKS - 1 - lax.div(n, OWN_L)) * OWN_L + lax.rem(n, OWN_L)


def late_kernel(pos_ref, q_ref, kv_ref, early_ref, wo_ref, k_ref, v_ref,
                out_e, out_l, wobuf, keep_k, keep_v,
                key, stat, late, recv_e, recv_l, own_e, own_l,
                wsem, krs, vrs, es, er, ls, lr, ges, ger, gls, glr):
    me = lax.axis_index('sp')
    start = me * SLOTS

    def reads(n):
        b = late_sequence(me, n)
        return (pltpu.make_async_copy(k_ref.at[b], keep_k.at[n], krs.at[n]),
                pltpu.make_async_copy(v_ref.at[b], keep_v.at[n], vrs.at[n]))

    def wo_copy(c):
        return pltpu.make_async_copy(wo_ref.at[:, pl.ds(pl.multiple_of(c * COLS, COLS), COLS)], wobuf.at[c], wsem.at[c])

    def remote(src, dst, send, recv, mask):
        return pltpu.make_async_remote_copy(src_ref=src, dst_ref=dst, send_sem=send, recv_sem=recv,
                                            device_id={'sp': flip(me, mask)}, device_id_type=MESH)

    def early_copy(m):
        return remote(early_ref.at[flip(me, m)], recv_e.at[m], es.at[m], er.at[m], m)

    def late_copy(m):
        return remote(late.at[m], recv_l.at[m], ls.at[m], lr.at[m], m)

    def start_reads(n, carry):
        for copy in reads(n):
            copy.start()
        return carry

    lax.fori_loop(0, 4, start_reads, 0)

    barrier = pltpu.get_barrier_semaphore()
    for m in range(1, RANKS):
        pl.semaphore_signal(barrier, inc=1, device_id={'sp': flip(me, m)}, device_id_type=MESH)
    pl.semaphore_wait(barrier, RANKS - 1)
    for m in range(RANKS - 1, 0, -1):
        early_copy(m).start()
    lax.fori_loop(4, AHEAD, start_reads, 0)
    recv_e[0] = early_ref[me]
    key[...] = head_columns()

    row16 = lax.broadcasted_iota(jnp.int32, (HEADS, 2 * KV), 0)
    col16 = lax.broadcasted_iota(jnp.int32, (HEADS, 2 * KV), 1)

    def attend(n):
        b = late_sequence(me, n)
        local = pos_ref[b] - start
        base = pl.ds(pl.multiple_of(b * HEADS, HEADS), HEADS)
        q = q_ref[base, :].astype(BF16)
        kv = kv_ref[base, :].astype(BF16)
        scores = scores_of(q, keep_k[n])
        live = key[...] < local * KV
        scores = jnp.where(live, scores, NEG_FILL)
        mine = jnp.where((local >= 0) & (local < SLOTS), row16 >> 1, 64)
        fresh = jnp.where(col16 == mine, scores_of(q, kv), NEG_FILL)
        fresh = jnp.max(fresh, axis=-1, keepdims=True)
        peak = jnp.maximum(jnp.max(scores, axis=-1, keepdims=True), fresh)
        e = jnp.where(live, jnp.exp(scores - peak), 0.0)
        ef = jnp.where(col16 == mine + KV, jnp.exp(fresh - peak), 0.0)
        total = jnp.sum(e, axis=-1, keepdims=True) + jnp.sum(ef, axis=-1, keepdims=True)
        out = jnp.dot(e.astype(BF16), keep_v[n], preferred_element_type=F32)
        out = out + jnp.dot(ef.astype(BF16), kv, preferred_element_type=F32)
        return out, stat_tile(peak, total)

    def group(g, carry):
        m = RANKS - 1 - g

        def pair(j, carry):
            n0 = g * OWN_L + 2 * j

            @pl.when(n0 + AHEAD < LATE)
            def _():
                for d in range(2):
                    start_reads(n0 + AHEAD + d, 0)

            @pl.when(n0 + AHEAD == LATE)
            def _():
                for c in range(CHUNKS):
                    wo_copy(c).start()

            for d in range(2):
                for copy in reads(n0 + d):
                    copy.wait()
            for d in range(2):
                out, st = attend(n0 + d)
                r = pl.multiple_of((2 * j + d) * HEADS, HEADS)
                late[m, pl.ds(r, HEADS), :] = out
                stat[pl.ds(r, HEADS), :] = st
            return carry

        lax.fori_loop(0, OWN_L // 2, pair, 0)
        late[m, pl.ds(OWN_L * HEADS, 8), pl.ds(0, OWN_L * HEADS)] = stat[...].T[0:8, :]

        @pl.when(g + 1 < RANKS)
        def _():
            late_copy(m).start()

        return carry

    def combine(recv, count):
        rows = count * HEADS
        stats = [recv[s, pl.ds(rows, 8), pl.ds(0, rows)].T for s in range(RANKS)]
        peak = stats[0][:, 0:1]
        for s in range(1, RANKS):
            peak = jnp.maximum(peak, stats[s][:, 0:1])
        total = jnp.zeros((rows, 1), F32)
        acc = jnp.zeros((rows, DIM), F32)
        for s in range(RANKS):
            w = jnp.exp(stats[s][:, 0:1] - peak)
            total = total + w * stats[s][:, 1:2]
            acc = acc + w * recv[s, pl.ds(0, rows), :]
        return acc / total

    def gather(own, out, gs, gr):
        size = own.shape[0]

        def place(rank):
            return out.at[pl.ds(pl.multiple_of(rank * size, size), size), :]

        def send(mask):
            return remote(own, place(me), gs.at[mask], gr.at[me], mask)

        def relay(mask):
            src = flip(me, mask)
            return remote(place(src), place(src), gs.at[mask + 1], gr.at[src], 1)

        def arrival(mask):
            src = flip(me, mask)
            return remote(own, place(src), gs.at[mask], gr.at[src], mask)

        def first():
            for mask in (6, 4, 2, 1):
                send(mask).start()
            out[pl.ds(pl.multiple_of(me * size, size), size), :] = own[...]

        def second():
            for mask in (2, 4, 6):
                arrival(mask).wait_recv()
                relay(mask).start()

        def last():
            for mask in (1, 3, 5, 7):
                arrival(mask).wait_recv()
            for mask in (6, 4, 2, 1):
                send(mask).wait_send()
            for mask in (2, 4, 6):
                relay(mask).wait_send()

        return first, second, last

    stages_e = gather(own_e, out_e, ges, ger)
    stages_l = gather(own_l, out_l, gls, glr)
    lax.fori_loop(0, RANKS - 1, group, 0)
    for m in range(RANKS - 1, 0, -1):
        early_copy(m).wait()
    own_e[...] = combine(recv_e, OWN_E)
    stages_e[0]()
    lax.fori_loop(RANKS - 1, RANKS, group, 0)
    recv_l[0] = late[0]
    for m in range(RANKS - 1, 0, -1):
        late_copy(m).wait()
    own_l[...] = combine(recv_l, OWN_L)
    stages_l[0]()
    stages_e[1]()
    stages_l[1]()
    for c in range(CHUNKS):
        wo_copy(c).wait()
    stages_e[2]()
    stages_l[2]()


def store_kernel(pos_ref, tok_ref, kv_ref, rows_e, rows_l, wobuf, keep_k_in, keep_v_in, ko_in, vo_in,
                 out_ref, keep_k, keep_v, ko_ref, vo_ref, attn, kws, vws):
    me = lax.axis_index('sp')
    start = me * SLOTS

    def writes(n):
        b = late_sequence(me, n)
        return (pltpu.make_async_copy(keep_k.at[n], ko_ref.at[b], kws), pltpu.make_async_copy(keep_v.at[n], vo_ref.at[b], vws))

    def step(n, carry):
        b = late_sequence(me, jnp.minimum(n, LATE - 1))
        local = pos_ref[b] - start

        @pl.when((n < LATE) & (local >= 0) & (local < SLOTS))
        def _():
            base = pl.multiple_of(b * 2 * KV, 2 * KV)
            insert(keep_k, n, local, kv_ref[pl.ds(base, KV), :])
            insert(keep_v, n, local, kv_ref[pl.ds(pl.multiple_of(base + KV, KV), KV), :])

        @pl.when(n >= 2)
        def _():
            for copy in writes(n - 2):
                copy.start()

        return carry

    lax.fori_loop(0, LATE + 2, step, 0)
    for h in range(HEADS):
        block = pl.ds(h * DIM, DIM)
        attn[pl.ds(0, EARLY), block] = rows_e[pl.ds(h, EARLY, stride=HEADS), :].astype(BF16)
        attn[pl.ds(EARLY, LATE), block] = rows_l[pl.ds(h, LATE, stride=HEADS), :].astype(BF16)
    for c in range(CHUNKS):
        block = pl.ds(c * COLS, COLS)
        y = jnp.dot(attn[...], wobuf[c], preferred_element_type=F32)
        out_ref[:, block] = (tok_ref[:, block].astype(F32) + y).astype(BF16)

    def drain(n, carry):
        for copy in writes(n):
            copy.wait()
        return carry

    lax.fori_loop(0, LATE, drain, 0)


def solution(mesh):
    cache_spec = P('dp', 'sp', None, None)
    hbm = pl.BlockSpec(memory_space=pltpu.HBM)
    vmem = pl.BlockSpec(memory_space=pltpu.VMEM)
    smem = pl.BlockSpec(memory_space=pltpu.SMEM)
    sds = jax.ShapeDtypeStruct
    flat = (SEQS, ROWS, DIM)
    dma = pltpu.SemaphoreType.DMA
    space = pltpu.VMEM

    def in_vmem(a):
        return pltpu.with_memory_space_constraint(a, pltpu.VMEM)

    def in_hbm(a):
        return pltpu.with_memory_space_constraint(a, pltpu.HBM)

    def device_step(tokens, positions, k_cache, v_cache, w_q, w_k, w_v, w_o, attn_norm, q_norm, k_norm):
        k_flat, v_flat = k_cache.reshape(flat), v_cache.reshape(flat)
        early, q, kv, new, k_out, v_out = pl.pallas_call(
            early_kernel,
            out_shape=(space((RANKS, PART_E, DIM), F32), space((SEQS * HEADS, DIM), F32), space((SEQS * 2 * KV, DIM), F32),
                       sds((SEQS * 2 * KV, DIM), BF16), sds(flat, BF16), sds(flat, BF16)),
            in_specs=[smem] + [vmem] * 5 + [hbm] * 5,
            out_specs=(vmem,) * 4 + (hbm,) * 2,
            scratch_shapes=[
                space((8, WIDTH, CHUNK), BF16), space((SEQS, WIDTH), BF16), space((SEQS, DIM), F32), space((SEQS, DIM), F32),
                space((HEADS, ROWS), jnp.int32), space((OWN_E * HEADS, DIM), F32),
                space((RING, ROWS, DIM), BF16), space((RING, ROWS, DIM), BF16),
                dma((8,)), dma((RING,)), dma((RING,)), dma((RING,)), dma((RING,)),
            ],
            compiler_params=pltpu.CompilerParams(vmem_limit_bytes=58 << 20),
        )(positions, tokens, frequencies(), attn_norm, q_norm, k_norm, in_hbm(w_q), in_hbm(w_k), in_hbm(w_v), in_hbm(k_flat), in_hbm(v_flat))
        rows_e, rows_l, wobuf, keep_k, keep_v = pl.pallas_call(
            late_kernel,
            out_shape=(space((EARLY * HEADS, DIM), F32), space((LATE * HEADS, DIM), F32), space((CHUNKS, WIDTH, COLS), BF16),
                       space((LATE, ROWS, DIM), BF16), space((LATE, ROWS, DIM), BF16)),
            in_specs=[smem] + [vmem] * 3 + [hbm] * 3,
            out_specs=(vmem,) * 5,
            scratch_shapes=[
                space((HEADS, ROWS), jnp.int32), space((OWN_L * HEADS, DIM), F32),
                space((RANKS, PART_L, DIM), F32), space((RANKS, PART_E, DIM), F32), space((RANKS, PART_L, DIM), F32),
                space((OWN_E * HEADS, DIM), F32), space((OWN_L * HEADS, DIM), F32),
                dma((CHUNKS,)), dma((LATE,)), dma((LATE,)), dma((RANKS,)), dma((RANKS,)), dma((RANKS,)), dma((RANKS,)),
                dma((RANKS,)), dma((RANKS,)), dma((RANKS,)), dma((RANKS,)),
            ],
            compiler_params=pltpu.CompilerParams(collective_id=0, has_side_effects=True, vmem_limit_bytes=3 << 20),
        )(positions, in_vmem(q), in_vmem(kv), in_vmem(early), in_hbm(w_o), in_hbm(k_flat), in_hbm(v_flat))
        block_out, _, _, k_out, v_out = pl.pallas_call(
            store_kernel,
            out_shape=(sds((SEQS, WIDTH), BF16), space((LATE, ROWS, DIM), BF16), space((LATE, ROWS, DIM), BF16), sds(flat, BF16), sds(flat, BF16)),
            in_specs=[smem] + [vmem] * 7 + [hbm] * 2,
            out_specs=(vmem, vmem, vmem, hbm, hbm),
            scratch_shapes=[space((SEQS, WIDTH), BF16), dma, dma],
            input_output_aliases={6: 1, 7: 2, 8: 3, 9: 4},
            compiler_params=pltpu.CompilerParams(vmem_limit_bytes=3 << 20),
        )(positions, tokens, in_vmem(kv), in_vmem(rows_e), in_vmem(rows_l), in_vmem(wobuf), in_vmem(keep_k), in_vmem(keep_v), k_out, v_out)
        return block_out, k_out.reshape(k_cache.shape), v_out.reshape(v_cache.shape), new.reshape(SEQS, 2, KV, DIM)

    return jax.shard_map(device_step, mesh=mesh, in_specs=(P('dp', None), P('dp'), cache_spec, cache_spec, P(), P(), P(), P(), P(), P(), P()), out_specs=(P('dp', None), cache_spec, cache_spec, P('dp', None, None, None)), check_vma=False)
```

```python
import jax
import jax.numpy as jnp
import numpy as np
from jax import lax
from jax.experimental import pallas as pl
from jax.experimental.pallas import tpu as pltpu
from jax.sharding import PartitionSpec as P

NORM_EPS = 1e-6
ROPE_THETA = 1000000.0
NEG_FILL = -1e30
F32 = jnp.float32
BF16 = jnp.bfloat16
MESH = pl.DeviceIdType.MESH

SEQS = 64
WIDTH = 2048
HEADS = 16
KV = 8
DIM = 128
SLOTS = 256
ROWS = SLOTS * KV
RANKS = 8
OWN = SEQS // RANKS
EARLY = 48
LATE = SEQS - EARLY
OWN_E = EARLY // RANKS
OWN_L = LATE // RANKS
PART_E = OWN_E * HEADS + 8
PART_L = OWN_L * HEADS + 8
CHUNK = 512
RING = 16
PAIRS = RING // 2
LAG = 3
COLS = 512
CHUNKS = WIDTH // COLS


def frequencies():
    half = ROPE_THETA ** (-np.arange(DIM // 2, dtype=np.float64) * 2.0 / DIM)
    return jnp.asarray(np.concatenate([half, half])[None, :], F32)


def head_columns():
    row = lax.broadcasted_iota(jnp.int32, (HEADS, ROWS), 0)
    col = lax.broadcasted_iota(jnp.int32, (HEADS, ROWS), 1)
    return jnp.where((col & (KV - 1)) == (row >> 1), col, 1 << 30)


def insert(buf, index, local, new):
    row = lax.broadcasted_iota(jnp.int32, (2 * KV, DIM), 0)
    slot = jnp.clip(local, 0, SLOTS - 1)
    first = jnp.where(local == slot, (slot & 1) * KV, 64)
    block = pl.ds(pl.multiple_of((slot >> 1) * 2 * KV, 2 * KV), 2 * KV)
    both = jnp.concatenate([new, new], axis=0)
    old = buf[index, block, :].astype(F32)
    hit = (row >= first) & (row < first + KV)
    buf[index, block, :] = jnp.where(hit, both, old).astype(BF16)


def scores_of(q, k):
    return lax.dot_general(q, k, (((1,), (1,)), ((), ())), preferred_element_type=F32) * (DIM ** -0.5)


def stat_tile(peak, total):
    lane = lax.broadcasted_iota(jnp.int32, (HEADS, DIM), 1)
    return jnp.where(lane == 0, peak, total)


def early_kernel(pos_ref, tok_ref, freq_ref, an_ref, qn_ref, kn_ref, wq_ref, wk_ref, wv_ref, k_ref, v_ref,
                 part_ref, q_scr, kv_scr, new_ref, ko_ref, vo_ref,
                 wbuf, hid, cos_scr, sin_scr, key, stat, kbuf, vbuf, wsem, krs, vrs, kws, vws):
    start = lax.axis_index('sp') * SLOTS

    def weight_copy(c):
        if c < 4:
            src = wq_ref.at[:, pl.ds(c * CHUNK, CHUNK)]
        elif c < 6:
            src = wk_ref.at[:, pl.ds((c - 4) * CHUNK, CHUNK)]
        else:
            src = wv_ref.at[:, pl.ds((c - 6) * CHUNK, CHUNK)]
        return pltpu.make_async_copy(src, wbuf.at[c], wsem.at[c])

    def pair_slots(i):
        return pl.ds(2 * lax.rem(i, PAIRS), 2)

    def reads(i):
        s = lax.rem(i, PAIRS)
        return (pltpu.make_async_copy(k_ref.at[pl.ds(2 * i, 2)], kbuf.at[pair_slots(i)], krs.at[s]),
                pltpu.make_async_copy(v_ref.at[pl.ds(2 * i, 2)], vbuf.at[pair_slots(i)], vrs.at[s]))

    def writes(i):
        s = lax.rem(i, PAIRS)
        return (pltpu.make_async_copy(kbuf.at[pair_slots(i)], ko_ref.at[pl.ds(2 * i, 2)], kws.at[s]),
                pltpu.make_async_copy(vbuf.at[pair_slots(i)], vo_ref.at[pl.ds(2 * i, 2)], vws.at[s]))

    for c in range(8):
        weight_copy(c).start()

    def first_reads(i, carry):
        for copy in reads(i):
            copy.start()
        return carry

    lax.fori_loop(0, PAIRS, first_reads, 0)

    x = tok_ref[...].astype(F32)
    scale = lax.rsqrt(jnp.mean(x * x, axis=-1, keepdims=True) + NORM_EPS)
    hid[...] = (x * scale * an_ref[...].astype(F32)[None, :]).astype(BF16)

    def fill(b, carry):
        cos_scr[pl.ds(b, 1), :] = jnp.full((1, DIM), pos_ref[b].astype(F32), F32)
        return carry

    lax.fori_loop(0, SEQS, fill, 0)
    angle = cos_scr[...] * freq_ref[...]
    lane = lax.broadcasted_iota(jnp.int32, (SEQS, DIM), 1)
    sin = jnp.sin(angle)
    cos_scr[...] = jnp.cos(angle)
    sin_scr[...] = jnp.where(lane < DIM // 2, -sin, sin)
    key[...] = head_columns()

    def norm_rope(y, gain):
        y = y * lax.rsqrt(jnp.mean(y * y, axis=-1, keepdims=True) + NORM_EPS) * gain
        return (y * cos_scr[...] + pltpu.roll(y, DIM // 2, 1) * sin_scr[...]).astype(BF16).astype(F32)

    qg = qn_ref[...].astype(F32)[None, :]
    kg = kn_ref[...].astype(F32)[None, :]
    for c in range(8):
        weight_copy(c).wait()
        y = jnp.dot(hid[...], wbuf[c], preferred_element_type=F32).astype(BF16).astype(F32)
        for j in range(CHUNK // DIM):
            yh = y[:, j * DIM:(j + 1) * DIM]
            if c < 4:
                q_scr[pl.ds(c * 4 + j, SEQS, stride=HEADS), :] = norm_rope(yh, qg)
            elif c < 6:
                kv_scr[pl.ds((c - 4) * 4 + j, SEQS, stride=2 * KV), :] = norm_rope(yh, kg)
            else:
                kv_scr[pl.ds(KV + (c - 6) * 4 + j, SEQS, stride=2 * KV), :] = yh
    new_ref[...] = kv_scr[...].astype(BF16)

    def attend(b):
        s = lax.rem(b, RING)
        local = pos_ref[b] - start
        q = q_scr[pl.ds(pl.multiple_of(b * HEADS, HEADS), HEADS), :].astype(BF16)
        scores = scores_of(q, kbuf[s])
        live = key[...] < (local + 1) * KV
        scores = jnp.where(live, scores, NEG_FILL)
        peak = jnp.max(scores, axis=-1, keepdims=True)
        e = jnp.where(live, jnp.exp(scores - peak), 0.0)
        total = jnp.sum(e, axis=-1, keepdims=True)
        out = jnp.dot(e.astype(BF16), vbuf[s], preferred_element_type=F32)
        return out, stat_tile(peak, total)

    def group(g, carry):
        def pair(j, carry):
            i = g * (OWN_E // 2) + j
            b0 = 2 * i

            @pl.when(i >= LAG)
            def _():
                for copy in writes(i - LAG):
                    copy.wait()

            @pl.when((i >= LAG) & (i - LAG + PAIRS < EARLY // 2))
            def _():
                for copy in reads(i - LAG + PAIRS):
                    copy.start()

            for copy in reads(i):
                copy.wait()
            for d in range(2):
                b = b0 + d
                s = lax.rem(b, RING)
                local = pos_ref[b] - start
                base = pl.multiple_of(b * 2 * KV, 2 * KV)
                insert(kbuf, s, local, kv_scr[pl.ds(base, KV), :])
                insert(vbuf, s, local, kv_scr[pl.ds(pl.multiple_of(base + KV, KV), KV), :])
            for d in range(2):
                out, st = attend(b0 + d)
                r = pl.multiple_of((2 * j + d) * HEADS, HEADS)
                part_ref[g, pl.ds(r, HEADS), :] = out
                stat[pl.ds(r, HEADS), :] = st
            for copy in writes(i):
                copy.start()
            return carry

        lax.fori_loop(0, OWN_E // 2, pair, 0)
        part_ref[g, pl.ds(OWN_E * HEADS, 8), pl.ds(0, OWN_E * HEADS)] = stat[...].T[0:8, :]
        return carry

    lax.fori_loop(0, RANKS, group, 0)
    for i in range(EARLY // 2 - LAG, EARLY // 2):
        for copy in writes(i):
            copy.wait()


def bit(value, place):
    if isinstance(value, int):
        return value // place % 2
    return lax.rem(lax.div(value, place), 2)


def flip(index, mask):
    return sum(lax.rem(bit(index, p) + bit(mask, p), 2) * p for p in (1, 2, 4))


def late_sequence(me, n):
    return EARLY + flip(me, RANKS - 1 - lax.div(n, OWN_L)) * OWN_L + lax.rem(n, OWN_L)


def late_kernel(pos_ref, q_ref, kv_ref, early_ref, wo_ref, k_ref, v_ref,
                out_e, out_l, wobuf, keep_k, keep_v,
                key, stat, late, recv_e, recv_l, own_e, own_l,
                wsem, krs, vrs, es, er, ls, lr, ges, ger, gls, glr):
    me = lax.axis_index('sp')
    start = me * SLOTS

    def reads(i):
        b = late_sequence(me, 2 * i)
        return (pltpu.make_async_copy(k_ref.at[pl.ds(b, 2)], keep_k.at[pl.ds(2 * i, 2)], krs.at[i]),
                pltpu.make_async_copy(v_ref.at[pl.ds(b, 2)], keep_v.at[pl.ds(2 * i, 2)], vrs.at[i]))

    def wo_copy(c):
        return pltpu.make_async_copy(wo_ref.at[:, pl.ds(pl.multiple_of(c * COLS, COLS), COLS)], wobuf.at[c], wsem.at[c])

    def remote(src, dst, send, recv, mask):
        return pltpu.make_async_remote_copy(src_ref=src, dst_ref=dst, send_sem=send, recv_sem=recv,
                                            device_id={'sp': flip(me, mask)}, device_id_type=MESH)

    def early_copy(m):
        return remote(early_ref.at[flip(me, m)], recv_e.at[m], es.at[m], er.at[m], m)

    def late_copy(m):
        return remote(late.at[m], recv_l.at[m], ls.at[m], lr.at[m], m)

    def start_reads(n, carry):
        for copy in reads(n):
            copy.start()
        return carry

    lax.fori_loop(0, 2, start_reads, 0)

    barrier = pltpu.get_barrier_semaphore()
    for m in range(1, RANKS):
        pl.semaphore_signal(barrier, inc=1, device_id={'sp': flip(me, m)}, device_id_type=MESH)
    pl.semaphore_wait(barrier, RANKS - 1)
    for m in range(RANKS - 1, 0, -1):
        early_copy(m).start()
    lax.fori_loop(2, LATE // 2, start_reads, 0)
    for c in range(CHUNKS):
        wo_copy(c).start()
    recv_e[0] = early_ref[me]
    key[...] = head_columns()

    row16 = lax.broadcasted_iota(jnp.int32, (HEADS, 2 * KV), 0)
    col16 = lax.broadcasted_iota(jnp.int32, (HEADS, 2 * KV), 1)

    def attend(n):
        b = late_sequence(me, n)
        local = pos_ref[b] - start
        base = pl.ds(pl.multiple_of(b * HEADS, HEADS), HEADS)
        q = q_ref[base, :].astype(BF16)
        kv = kv_ref[base, :].astype(BF16)
        scores = scores_of(q, keep_k[n])
        live = key[...] < local * KV
        scores = jnp.where(live, scores, NEG_FILL)
        mine = jnp.where((local >= 0) & (local < SLOTS), row16 >> 1, 64)
        fresh = jnp.where(col16 == mine, scores_of(q, kv), NEG_FILL)
        fresh = jnp.max(fresh, axis=-1, keepdims=True)
        peak = jnp.maximum(jnp.max(scores, axis=-1, keepdims=True), fresh)
        e = jnp.where(live, jnp.exp(scores - peak), 0.0)
        ef = jnp.where(col16 == mine + KV, jnp.exp(fresh - peak), 0.0)
        total = jnp.sum(e, axis=-1, keepdims=True) + jnp.sum(ef, axis=-1, keepdims=True)
        out = jnp.dot(e.astype(BF16), keep_v[n], preferred_element_type=F32)
        out = out + jnp.dot(ef.astype(BF16), kv, preferred_element_type=F32)
        return out, stat_tile(peak, total)

    def group(g, carry):
        m = RANKS - 1 - g

        def pair(j, carry):
            n0 = g * OWN_L + 2 * j

            for copy in reads(g * (OWN_L // 2) + j):
                copy.wait()
            for d in range(2):
                out, st = attend(n0 + d)
                r = pl.multiple_of((2 * j + d) * HEADS, HEADS)
                late[m, pl.ds(r, HEADS), :] = out
                stat[pl.ds(r, HEADS), :] = st
            return carry

        lax.fori_loop(0, OWN_L // 2, pair, 0)
        late[m, pl.ds(OWN_L * HEADS, 8), pl.ds(0, OWN_L * HEADS)] = stat[...].T[0:8, :]

        @pl.when(g + 1 < RANKS)
        def _():
            late_copy(m).start()

        return carry

    def combine(recv, count):
        rows = count * HEADS
        stats = [recv[s, pl.ds(rows, 8), pl.ds(0, rows)].T for s in range(RANKS)]
        peak = stats[0][:, 0:1]
        for s in range(1, RANKS):
            peak = jnp.maximum(peak, stats[s][:, 0:1])
        total = jnp.zeros((rows, 1), F32)
        acc = jnp.zeros((rows, DIM), F32)
        for s in range(RANKS):
            w = jnp.exp(stats[s][:, 0:1] - peak)
            total = total + w * stats[s][:, 1:2]
            acc = acc + w * recv[s, pl.ds(0, rows), :]
        return acc / total

    def gather(own, out, gs, gr):
        size = own.shape[0]

        def place(rank):
            return out.at[pl.ds(pl.multiple_of(rank * size, size), size), :]

        def send(mask):
            return remote(own, place(me), gs.at[mask], gr.at[me], mask)

        def relay(mask):
            src = flip(me, mask)
            return remote(place(src), place(src), gs.at[mask + 1], gr.at[src], 1)

        def arrival(mask):
            src = flip(me, mask)
            return remote(own, place(src), gs.at[mask], gr.at[src], mask)

        def first():
            for mask in (6, 4, 2, 1):
                send(mask).start()
            out[pl.ds(pl.multiple_of(me * size, size), size), :] = own[...]

        def second():
            for mask in (2, 4, 6):
                arrival(mask).wait_recv()
                relay(mask).start()

        def last():
            for mask in (1, 3, 5, 7):
                arrival(mask).wait_recv()
            for mask in (6, 4, 2, 1):
                send(mask).wait_send()
            for mask in (2, 4, 6):
                relay(mask).wait_send()

        return first, second, last

    stages_e = gather(own_e, out_e, ges, ger)
    stages_l = gather(own_l, out_l, gls, glr)
    lax.fori_loop(0, RANKS - 1, group, 0)
    for m in range(RANKS - 1, 0, -1):
        early_copy(m).wait()
    own_e[...] = combine(recv_e, OWN_E)
    stages_e[0]()
    lax.fori_loop(RANKS - 1, RANKS, group, 0)
    recv_l[0] = late[0]
    for m in range(RANKS - 1, 0, -1):
        late_copy(m).wait()
    own_l[...] = combine(recv_l, OWN_L)
    stages_l[0]()
    stages_e[1]()
    stages_l[1]()
    for c in range(CHUNKS):
        wo_copy(c).wait()
    stages_e[2]()
    stages_l[2]()


def store_kernel(pos_ref, tok_ref, kv_ref, rows_e, rows_l, wobuf, keep_k_in, keep_v_in, ko_in, vo_in,
                 out_ref, keep_k, keep_v, ko_ref, vo_ref, attn, kws, vws):
    me = lax.axis_index('sp')
    start = me * SLOTS

    def writes(i):
        b = late_sequence(me, 2 * i)
        return (pltpu.make_async_copy(keep_k.at[pl.ds(2 * i, 2)], ko_ref.at[pl.ds(b, 2)], kws),
                pltpu.make_async_copy(keep_v.at[pl.ds(2 * i, 2)], vo_ref.at[pl.ds(b, 2)], vws))

    def step(n, carry):
        b = late_sequence(me, jnp.minimum(n, LATE - 1))
        local = pos_ref[b] - start

        @pl.when((n < LATE) & (local >= 0) & (local < SLOTS))
        def _():
            base = pl.multiple_of(b * 2 * KV, 2 * KV)
            insert(keep_k, n, local, kv_ref[pl.ds(base, KV), :])
            insert(keep_v, n, local, kv_ref[pl.ds(pl.multiple_of(base + KV, KV), KV), :])

        @pl.when((n >= 3) & (lax.rem(n, 2) == 1))
        def _():
            for copy in writes(lax.div(n - 3, 2)):
                copy.start()

        return carry

    lax.fori_loop(0, LATE + 2, step, 0)
    for h in range(HEADS):
        block = pl.ds(h * DIM, DIM)
        attn[pl.ds(0, EARLY), block] = rows_e[pl.ds(h, EARLY, stride=HEADS), :].astype(BF16)
        attn[pl.ds(EARLY, LATE), block] = rows_l[pl.ds(h, LATE, stride=HEADS), :].astype(BF16)
    for c in range(CHUNKS):
        block = pl.ds(c * COLS, COLS)
        y = jnp.dot(attn[...], wobuf[c], preferred_element_type=F32)
        out_ref[:, block] = (tok_ref[:, block].astype(F32) + y).astype(BF16)

    def drain(n, carry):
        for copy in writes(n):
            copy.wait()
        return carry

    lax.fori_loop(0, LATE // 2, drain, 0)


def solution(mesh):
    cache_spec = P('dp', 'sp', None, None)
    hbm = pl.BlockSpec(memory_space=pltpu.HBM)
    vmem = pl.BlockSpec(memory_space=pltpu.VMEM)
    smem = pl.BlockSpec(memory_space=pltpu.SMEM)
    sds = jax.ShapeDtypeStruct
    flat = (SEQS, ROWS, DIM)
    dma = pltpu.SemaphoreType.DMA
    space = pltpu.VMEM

    def in_vmem(a):
        return pltpu.with_memory_space_constraint(a, pltpu.VMEM)

    def in_hbm(a):
        return pltpu.with_memory_space_constraint(a, pltpu.HBM)

    def device_step(tokens, positions, k_cache, v_cache, w_q, w_k, w_v, w_o, attn_norm, q_norm, k_norm):
        k_flat, v_flat = k_cache.reshape(flat), v_cache.reshape(flat)
        early, q, kv, new, k_out, v_out = pl.pallas_call(
            early_kernel,
            out_shape=(space((RANKS, PART_E, DIM), F32), space((SEQS * HEADS, DIM), F32), space((SEQS * 2 * KV, DIM), F32),
                       sds((SEQS * 2 * KV, DIM), BF16), sds(flat, BF16), sds(flat, BF16)),
            in_specs=[smem] + [vmem] * 5 + [hbm] * 5,
            out_specs=(vmem,) * 4 + (hbm,) * 2,
            scratch_shapes=[
                space((8, WIDTH, CHUNK), BF16), space((SEQS, WIDTH), BF16), space((SEQS, DIM), F32), space((SEQS, DIM), F32),
                space((HEADS, ROWS), jnp.int32), space((OWN_E * HEADS, DIM), F32),
                space((RING, ROWS, DIM), BF16), space((RING, ROWS, DIM), BF16),
                dma((8,)), dma((PAIRS,)), dma((PAIRS,)), dma((PAIRS,)), dma((PAIRS,)),
            ],
            compiler_params=pltpu.CompilerParams(vmem_limit_bytes=58 << 20),
        )(positions, tokens, frequencies(), attn_norm, q_norm, k_norm, in_hbm(w_q), in_hbm(w_k), in_hbm(w_v), in_hbm(k_flat), in_hbm(v_flat))
        rows_e, rows_l, wobuf, keep_k, keep_v = pl.pallas_call(
            late_kernel,
            out_shape=(space((EARLY * HEADS, DIM), F32), space((LATE * HEADS, DIM), F32), space((CHUNKS, WIDTH, COLS), BF16),
                       space((LATE, ROWS, DIM), BF16), space((LATE, ROWS, DIM), BF16)),
            in_specs=[smem] + [vmem] * 3 + [hbm] * 3,
            out_specs=(vmem,) * 5,
            scratch_shapes=[
                space((HEADS, ROWS), jnp.int32), space((OWN_L * HEADS, DIM), F32),
                space((RANKS, PART_L, DIM), F32), space((RANKS, PART_E, DIM), F32), space((RANKS, PART_L, DIM), F32),
                space((OWN_E * HEADS, DIM), F32), space((OWN_L * HEADS, DIM), F32),
                dma((CHUNKS,)), dma((LATE // 2,)), dma((LATE // 2,)), dma((RANKS,)), dma((RANKS,)), dma((RANKS,)), dma((RANKS,)),
                dma((RANKS,)), dma((RANKS,)), dma((RANKS,)), dma((RANKS,)),
            ],
            compiler_params=pltpu.CompilerParams(collective_id=0, has_side_effects=True, vmem_limit_bytes=3 << 20),
        )(positions, in_vmem(q), in_vmem(kv), in_vmem(early), in_hbm(w_o), in_hbm(k_flat), in_hbm(v_flat))
        block_out, _, _, k_out, v_out = pl.pallas_call(
            store_kernel,
            out_shape=(sds((SEQS, WIDTH), BF16), space((LATE, ROWS, DIM), BF16), space((LATE, ROWS, DIM), BF16), sds(flat, BF16), sds(flat, BF16)),
            in_specs=[smem] + [vmem] * 7 + [hbm] * 2,
            out_specs=(vmem, vmem, vmem, hbm, hbm),
            scratch_shapes=[space((SEQS, WIDTH), BF16), dma, dma],
            input_output_aliases={6: 1, 7: 2, 8: 3, 9: 4},
            compiler_params=pltpu.CompilerParams(vmem_limit_bytes=3 << 20),
        )(positions, tokens, in_vmem(kv), in_vmem(rows_e), in_vmem(rows_l), in_vmem(wobuf), in_vmem(keep_k), in_vmem(keep_v), k_out, v_out)
        return block_out, k_out.reshape(k_cache.shape), v_out.reshape(v_cache.shape), new.reshape(SEQS, 2, KV, DIM)

    return jax.shard_map(device_step, mesh=mesh, in_specs=(P('dp', None), P('dp'), cache_spec, cache_spec, P(), P(), P(), P(), P(), P(), P()), out_specs=(P('dp', None), cache_spec, cache_spec, P('dp', None, None, None)), check_vma=False)
```

```python
import jax
import jax.numpy as jnp
import numpy as np
from jax import lax
from jax.experimental import pallas as pl
from jax.experimental.pallas import tpu as pltpu
from jax.sharding import PartitionSpec as P

NORM_EPS = 1e-6
ROPE_THETA = 1000000.0
NEG_FILL = -1e30
F32 = jnp.float32
BF16 = jnp.bfloat16
MESH = pl.DeviceIdType.MESH

SEQS = 64
WIDTH = 2048
HEADS = 16
KV = 8
DIM = 128
SLOTS = 256
ROWS = SLOTS * KV
RANKS = 8
OWN = SEQS // RANKS
EARLY = 48
LATE = SEQS - EARLY
OWN_E = EARLY // RANKS
OWN_L = LATE // RANKS
PART_E = OWN_E * HEADS + 8
PART_L = OWN_L * HEADS + 8
CHUNK = 512
RING = 24
PAIRS = RING // 2
LAG = 5
COLS = 512
CHUNKS = WIDTH // COLS


def frequencies():
    half = ROPE_THETA ** (-np.arange(DIM // 2, dtype=np.float64) * 2.0 / DIM)
    return jnp.asarray(np.concatenate([half, half])[None, :], F32)


def head_columns():
    row = lax.broadcasted_iota(jnp.int32, (HEADS, ROWS), 0)
    col = lax.broadcasted_iota(jnp.int32, (HEADS, ROWS), 1)
    return jnp.where((col & (KV - 1)) == (row >> 1), col, 1 << 30)


def insert(buf, index, local, new):
    row = lax.broadcasted_iota(jnp.int32, (2 * KV, DIM), 0)
    slot = jnp.clip(local, 0, SLOTS - 1)
    first = jnp.where(local == slot, (slot & 1) * KV, 64)
    block = pl.ds(pl.multiple_of((slot >> 1) * 2 * KV, 2 * KV), 2 * KV)
    both = jnp.concatenate([new, new], axis=0)
    old = buf[index, block, :].astype(F32)
    hit = (row >= first) & (row < first + KV)
    buf[index, block, :] = jnp.where(hit, both, old).astype(BF16)


def scores_of(q, k):
    return lax.dot_general(q, k, (((1,), (1,)), ((), ())), preferred_element_type=F32) * (DIM ** -0.5)


def stat_tile(peak, total):
    lane = lax.broadcasted_iota(jnp.int32, (HEADS, DIM), 1)
    return jnp.where(lane == 0, peak, total)


def early_kernel(pos_ref, tok_ref, freq_ref, an_ref, qn_ref, kn_ref, wq_ref, wk_ref, wv_ref, k_ref, v_ref,
                 part_ref, q_scr, kv_scr, new_ref, ko_ref, vo_ref,
                 wbuf, hid, cos_scr, sin_scr, key, stat, kbuf, vbuf, wsem, krs, vrs, kws, vws):
    start = lax.axis_index('sp') * SLOTS

    def weight_copy(c):
        if c < 4:
            src = wq_ref.at[:, pl.ds(c * CHUNK, CHUNK)]
        elif c < 6:
            src = wk_ref.at[:, pl.ds((c - 4) * CHUNK, CHUNK)]
        else:
            src = wv_ref.at[:, pl.ds((c - 6) * CHUNK, CHUNK)]
        return pltpu.make_async_copy(src, wbuf.at[c], wsem.at[c])

    def pair_slots(i):
        return pl.ds(2 * lax.rem(i, PAIRS), 2)

    def reads(i):
        s = lax.rem(i, PAIRS)
        return (pltpu.make_async_copy(k_ref.at[pl.ds(2 * i, 2)], kbuf.at[pair_slots(i)], krs.at[s]),
                pltpu.make_async_copy(v_ref.at[pl.ds(2 * i, 2)], vbuf.at[pair_slots(i)], vrs.at[s]))

    def writes(i):
        s = lax.rem(i, PAIRS)
        return (pltpu.make_async_copy(kbuf.at[pair_slots(i)], ko_ref.at[pl.ds(2 * i, 2)], kws.at[s]),
                pltpu.make_async_copy(vbuf.at[pair_slots(i)], vo_ref.at[pl.ds(2 * i, 2)], vws.at[s]))

    for c in range(8):
        weight_copy(c).start()

    def first_reads(i, carry):
        for copy in reads(i):
            copy.start()
        return carry

    lax.fori_loop(0, PAIRS, first_reads, 0)

    x = tok_ref[...].astype(F32)
    scale = lax.rsqrt(jnp.mean(x * x, axis=-1, keepdims=True) + NORM_EPS)
    hid[...] = (x * scale * an_ref[...].astype(F32)[None, :]).astype(BF16)

    def fill(b, carry):
        cos_scr[pl.ds(b, 1), :] = jnp.full((1, DIM), pos_ref[b].astype(F32), F32)
        return carry

    lax.fori_loop(0, SEQS, fill, 0)
    angle = cos_scr[...] * freq_ref[...]
    lane = lax.broadcasted_iota(jnp.int32, (SEQS, DIM), 1)
    sin = jnp.sin(angle)
    cos_scr[...] = jnp.cos(angle)
    sin_scr[...] = jnp.where(lane < DIM // 2, -sin, sin)
    key[...] = head_columns()

    def norm_rope(y, gain):
        y = y * lax.rsqrt(jnp.mean(y * y, axis=-1, keepdims=True) + NORM_EPS) * gain
        return (y * cos_scr[...] + pltpu.roll(y, DIM // 2, 1) * sin_scr[...]).astype(BF16).astype(F32)

    qg = qn_ref[...].astype(F32)[None, :]
    kg = kn_ref[...].astype(F32)[None, :]
    for c in range(8):
        weight_copy(c).wait()
        y = jnp.dot(hid[...], wbuf[c], preferred_element_type=F32).astype(BF16).astype(F32)
        for j in range(CHUNK // DIM):
            yh = y[:, j * DIM:(j + 1) * DIM]
            if c < 4:
                q_scr[pl.ds(c * 4 + j, SEQS, stride=HEADS), :] = norm_rope(yh, qg)
            elif c < 6:
                kv_scr[pl.ds((c - 4) * 4 + j, SEQS, stride=2 * KV), :] = norm_rope(yh, kg)
            else:
                kv_scr[pl.ds(KV + (c - 6) * 4 + j, SEQS, stride=2 * KV), :] = yh
    new_ref[...] = kv_scr[...].astype(BF16)

    def attend(b):
        s = lax.rem(b, RING)
        local = pos_ref[b] - start
        q = q_scr[pl.ds(pl.multiple_of(b * HEADS, HEADS), HEADS), :].astype(BF16)
        scores = scores_of(q, kbuf[s])
        live = key[...] < (local + 1) * KV
        scores = jnp.where(live, scores, NEG_FILL)
        peak = jnp.max(scores, axis=-1, keepdims=True)
        e = jnp.where(live, jnp.exp(scores - peak), 0.0)
        total = jnp.sum(e, axis=-1, keepdims=True)
        out = jnp.dot(e.astype(BF16), vbuf[s], preferred_element_type=F32)
        return out, stat_tile(peak, total)

    def group(g, carry):
        def pair(j, carry):
            i = g * (OWN_E // 2) + j
            b0 = 2 * i

            @pl.when(i >= LAG)
            def _():
                for copy in writes(i - LAG):
                    copy.wait()

            @pl.when((i >= LAG) & (i - LAG + PAIRS < EARLY // 2))
            def _():
                for copy in reads(i - LAG + PAIRS):
                    copy.start()

            for copy in reads(i):
                copy.wait()
            for d in range(2):
                b = b0 + d
                s = lax.rem(b, RING)
                local = pos_ref[b] - start
                base = pl.multiple_of(b * 2 * KV, 2 * KV)
                insert(kbuf, s, local, kv_scr[pl.ds(base, KV), :])
                insert(vbuf, s, local, kv_scr[pl.ds(pl.multiple_of(base + KV, KV), KV), :])
            for d in range(2):
                out, st = attend(b0 + d)
                r = pl.multiple_of((2 * j + d) * HEADS, HEADS)
                part_ref[g, pl.ds(r, HEADS), :] = out
                stat[pl.ds(r, HEADS), :] = st
            for copy in writes(i):
                copy.start()
            return carry

        lax.fori_loop(0, OWN_E // 2, pair, 0)
        part_ref[g, pl.ds(OWN_E * HEADS, 8), pl.ds(0, OWN_E * HEADS)] = stat[...].T[0:8, :]
        return carry

    lax.fori_loop(0, RANKS, group, 0)
    for i in range(EARLY // 2 - LAG, EARLY // 2):
        for copy in writes(i):
            copy.wait()


def bit(value, place):
    if isinstance(value, int):
        return value // place % 2
    return lax.rem(lax.div(value, place), 2)


def flip(index, mask):
    return sum(lax.rem(bit(index, p) + bit(mask, p), 2) * p for p in (1, 2, 4))


def late_sequence(me, n):
    return EARLY + flip(me, RANKS - 1 - lax.div(n, OWN_L)) * OWN_L + lax.rem(n, OWN_L)


def late_kernel(pos_ref, q_ref, kv_ref, early_ref, wo_ref, k_ref, v_ref,
                out_e, out_l, wobuf, keep_k, keep_v,
                key, stat, late, recv_e, recv_l, own_e, own_l,
                wsem, krs, vrs, es, er, ls, lr, ges, ger, gls, glr):
    me = lax.axis_index('sp')
    start = me * SLOTS

    def reads(i):
        b = late_sequence(me, 2 * i)
        return (pltpu.make_async_copy(k_ref.at[pl.ds(b, 2)], keep_k.at[pl.ds(2 * i, 2)], krs.at[i]),
                pltpu.make_async_copy(v_ref.at[pl.ds(b, 2)], keep_v.at[pl.ds(2 * i, 2)], vrs.at[i]))

    def wo_copy(c):
        return pltpu.make_async_copy(wo_ref.at[:, pl.ds(pl.multiple_of(c * COLS, COLS), COLS)], wobuf.at[c], wsem.at[c])

    def remote(src, dst, send, recv, mask):
        return pltpu.make_async_remote_copy(src_ref=src, dst_ref=dst, send_sem=send, recv_sem=recv,
                                            device_id={'sp': flip(me, mask)}, device_id_type=MESH)

    def early_copy(m):
        return remote(early_ref.at[flip(me, m)], recv_e.at[m], es.at[m], er.at[m], m)

    def late_copy(m):
        return remote(late.at[m], recv_l.at[m], ls.at[m], lr.at[m], m)

    def start_reads(n, carry):
        for copy in reads(n):
            copy.start()
        return carry

    barrier = pltpu.get_barrier_semaphore()
    for m in range(1, RANKS):
        pl.semaphore_signal(barrier, inc=1, device_id={'sp': flip(me, m)}, device_id_type=MESH)
    lax.fori_loop(0, 2, start_reads, 0)
    key[...] = head_columns()
    pl.semaphore_wait(barrier, RANKS - 1)
    for m in range(RANKS - 1, 0, -1):
        early_copy(m).start()
    lax.fori_loop(2, LATE // 2, start_reads, 0)
    for c in range(CHUNKS):
        wo_copy(c).start()
    recv_e[0] = early_ref[me]

    row16 = lax.broadcasted_iota(jnp.int32, (HEADS, 2 * KV), 0)
    col16 = lax.broadcasted_iota(jnp.int32, (HEADS, 2 * KV), 1)

    def attend(n):
        b = late_sequence(me, n)
        local = pos_ref[b] - start
        base = pl.ds(pl.multiple_of(b * HEADS, HEADS), HEADS)
        q = q_ref[base, :].astype(BF16)
        kv = kv_ref[base, :].astype(BF16)
        scores = scores_of(q, keep_k[n])
        live = key[...] < local * KV
        scores = jnp.where(live, scores, NEG_FILL)
        mine = jnp.where((local >= 0) & (local < SLOTS), row16 >> 1, 64)
        fresh = jnp.where(col16 == mine, scores_of(q, kv), NEG_FILL)
        fresh = jnp.max(fresh, axis=-1, keepdims=True)
        peak = jnp.maximum(jnp.max(scores, axis=-1, keepdims=True), fresh)
        e = jnp.where(live, jnp.exp(scores - peak), 0.0)
        ef = jnp.where(col16 == mine + KV, jnp.exp(fresh - peak), 0.0)
        total = jnp.sum(e, axis=-1, keepdims=True) + jnp.sum(ef, axis=-1, keepdims=True)
        out = jnp.dot(e.astype(BF16), keep_v[n], preferred_element_type=F32)
        out = out + jnp.dot(ef.astype(BF16), kv, preferred_element_type=F32)
        return out, stat_tile(peak, total)

    def group(g, carry):
        m = RANKS - 1 - g

        def pair(j, carry):
            n0 = g * OWN_L + 2 * j

            for copy in reads(g * (OWN_L // 2) + j):
                copy.wait()
            for d in range(2):
                out, st = attend(n0 + d)
                r = pl.multiple_of((2 * j + d) * HEADS, HEADS)
                late[m, pl.ds(r, HEADS), :] = out
                stat[pl.ds(r, HEADS), :] = st
            return carry

        lax.fori_loop(0, OWN_L // 2, pair, 0)
        late[m, pl.ds(OWN_L * HEADS, 8), pl.ds(0, OWN_L * HEADS)] = stat[...].T[0:8, :]

        @pl.when(g + 1 < RANKS)
        def _():
            late_copy(m).start()

        return carry

    def combine(recv, count):
        rows = count * HEADS
        stats = [recv[s, pl.ds(rows, 8), pl.ds(0, rows)].T for s in range(RANKS)]
        peak = stats[0][:, 0:1]
        for s in range(1, RANKS):
            peak = jnp.maximum(peak, stats[s][:, 0:1])
        total = jnp.zeros((rows, 1), F32)
        acc = jnp.zeros((rows, DIM), F32)
        for s in range(RANKS):
            w = jnp.exp(stats[s][:, 0:1] - peak)
            total = total + w * stats[s][:, 1:2]
            acc = acc + w * recv[s, pl.ds(0, rows), :]
        return acc / total

    def gather(own, out, gs, gr):
        size = own.shape[0]

        def place(rank):
            return out.at[pl.ds(pl.multiple_of(rank * size, size), size), :]

        def send(mask):
            return remote(own, place(me), gs.at[mask], gr.at[me], mask)

        def relay(mask):
            src = flip(me, mask)
            return remote(place(src), place(src), gs.at[mask + 1], gr.at[src], 1)

        def arrival(mask):
            src = flip(me, mask)
            return remote(own, place(src), gs.at[mask], gr.at[src], mask)

        def first():
            for mask in (6, 4, 2, 1):
                send(mask).start()
            out[pl.ds(pl.multiple_of(me * size, size), size), :] = own[...]

        def second():
            for mask in (2, 4, 6):
                arrival(mask).wait_recv()
                relay(mask).start()

        def last():
            for mask in (1, 3, 5, 7):
                arrival(mask).wait_recv()
            for mask in (6, 4, 2, 1):
                send(mask).wait_send()
            for mask in (2, 4, 6):
                relay(mask).wait_send()

        return first, second, last

    stages_e = gather(own_e, out_e, ges, ger)
    stages_l = gather(own_l, out_l, gls, glr)
    lax.fori_loop(0, RANKS - 1, group, 0)
    for m in range(RANKS - 1, 0, -1):
        early_copy(m).wait()
    own_e[...] = combine(recv_e, OWN_E)
    stages_e[0]()
    lax.fori_loop(RANKS - 1, RANKS, group, 0)
    recv_l[0] = late[0]
    for m in range(RANKS - 1, 0, -1):
        late_copy(m).wait()
    own_l[...] = combine(recv_l, OWN_L)
    stages_l[0]()
    stages_e[1]()
    stages_l[1]()
    for c in range(CHUNKS):
        wo_copy(c).wait()
    stages_e[2]()
    stages_l[2]()


def store_kernel(pos_ref, tok_ref, kv_ref, rows_e, rows_l, wobuf, keep_k_in, keep_v_in, ko_in, vo_in,
                 out_ref, keep_k, keep_v, ko_ref, vo_ref, attn, kws, vws):
    me = lax.axis_index('sp')
    start = me * SLOTS

    def writes(i):
        b = late_sequence(me, 2 * i)
        return (pltpu.make_async_copy(keep_k.at[pl.ds(2 * i, 2)], ko_ref.at[pl.ds(b, 2)], kws),
                pltpu.make_async_copy(keep_v.at[pl.ds(2 * i, 2)], vo_ref.at[pl.ds(b, 2)], vws))

    def step(n, carry):
        b = late_sequence(me, jnp.minimum(n, LATE - 1))
        local = pos_ref[b] - start

        @pl.when((n < LATE) & (local >= 0) & (local < SLOTS))
        def _():
            base = pl.multiple_of(b * 2 * KV, 2 * KV)
            insert(keep_k, n, local, kv_ref[pl.ds(base, KV), :])
            insert(keep_v, n, local, kv_ref[pl.ds(pl.multiple_of(base + KV, KV), KV), :])

        @pl.when((n >= 3) & (lax.rem(n, 2) == 1))
        def _():
            for copy in writes(lax.div(n - 3, 2)):
                copy.start()

        return carry

    lax.fori_loop(0, LATE + 2, step, 0)
    for h in range(HEADS):
        block = pl.ds(h * DIM, DIM)
        attn[pl.ds(0, EARLY), block] = rows_e[pl.ds(h, EARLY, stride=HEADS), :].astype(BF16)
        attn[pl.ds(EARLY, LATE), block] = rows_l[pl.ds(h, LATE, stride=HEADS), :].astype(BF16)
    for c in range(CHUNKS):
        block = pl.ds(c * COLS, COLS)
        y = jnp.dot(attn[...], wobuf[c], preferred_element_type=F32)
        out_ref[:, block] = (tok_ref[:, block].astype(F32) + y).astype(BF16)

    def drain(n, carry):
        for copy in writes(n):
            copy.wait()
        return carry

    lax.fori_loop(0, LATE // 2, drain, 0)


def solution(mesh):
    cache_spec = P('dp', 'sp', None, None)
    hbm = pl.BlockSpec(memory_space=pltpu.HBM)
    vmem = pl.BlockSpec(memory_space=pltpu.VMEM)
    smem = pl.BlockSpec(memory_space=pltpu.SMEM)
    sds = jax.ShapeDtypeStruct
    flat = (SEQS, ROWS, DIM)
    dma = pltpu.SemaphoreType.DMA
    space = pltpu.VMEM

    def in_vmem(a):
        return pltpu.with_memory_space_constraint(a, pltpu.VMEM)

    def in_hbm(a):
        return pltpu.with_memory_space_constraint(a, pltpu.HBM)

    def device_step(tokens, positions, k_cache, v_cache, w_q, w_k, w_v, w_o, attn_norm, q_norm, k_norm):
        k_flat, v_flat = k_cache.reshape(flat), v_cache.reshape(flat)
        early, q, kv, new, k_out, v_out = pl.pallas_call(
            early_kernel,
            out_shape=(space((RANKS, PART_E, DIM), F32), space((SEQS * HEADS, DIM), F32), space((SEQS * 2 * KV, DIM), F32),
                       sds((SEQS * 2 * KV, DIM), BF16), sds(flat, BF16), sds(flat, BF16)),
            in_specs=[smem] + [vmem] * 5 + [hbm] * 5,
            out_specs=(vmem,) * 4 + (hbm,) * 2,
            scratch_shapes=[
                space((8, WIDTH, CHUNK), BF16), space((SEQS, WIDTH), BF16), space((SEQS, DIM), F32), space((SEQS, DIM), F32),
                space((HEADS, ROWS), jnp.int32), space((OWN_E * HEADS, DIM), F32),
                space((RING, ROWS, DIM), BF16), space((RING, ROWS, DIM), BF16),
                dma((8,)), dma((PAIRS,)), dma((PAIRS,)), dma((PAIRS,)), dma((PAIRS,)),
            ],
            compiler_params=pltpu.CompilerParams(vmem_limit_bytes=58 << 20),
        )(positions, tokens, frequencies(), attn_norm, q_norm, k_norm, in_hbm(w_q), in_hbm(w_k), in_hbm(w_v), in_hbm(k_flat), in_hbm(v_flat))
        rows_e, rows_l, wobuf, keep_k, keep_v = pl.pallas_call(
            late_kernel,
            out_shape=(space((EARLY * HEADS, DIM), F32), space((LATE * HEADS, DIM), F32), space((CHUNKS, WIDTH, COLS), BF16),
                       space((LATE, ROWS, DIM), BF16), space((LATE, ROWS, DIM), BF16)),
            in_specs=[smem] + [vmem] * 3 + [hbm] * 3,
            out_specs=(vmem,) * 5,
            scratch_shapes=[
                space((HEADS, ROWS), jnp.int32), space((OWN_L * HEADS, DIM), F32),
                space((RANKS, PART_L, DIM), F32), space((RANKS, PART_E, DIM), F32), space((RANKS, PART_L, DIM), F32),
                space((OWN_E * HEADS, DIM), F32), space((OWN_L * HEADS, DIM), F32),
                dma((CHUNKS,)), dma((LATE // 2,)), dma((LATE // 2,)), dma((RANKS,)), dma((RANKS,)), dma((RANKS,)), dma((RANKS,)),
                dma((RANKS,)), dma((RANKS,)), dma((RANKS,)), dma((RANKS,)),
            ],
            compiler_params=pltpu.CompilerParams(collective_id=0, has_side_effects=True, vmem_limit_bytes=3 << 20),
        )(positions, in_vmem(q), in_vmem(kv), in_vmem(early), in_hbm(w_o), in_hbm(k_flat), in_hbm(v_flat))
        block_out, _, _, k_out, v_out = pl.pallas_call(
            store_kernel,
            out_shape=(sds((SEQS, WIDTH), BF16), space((LATE, ROWS, DIM), BF16), space((LATE, ROWS, DIM), BF16), sds(flat, BF16), sds(flat, BF16)),
            in_specs=[smem] + [vmem] * 7 + [hbm] * 2,
            out_specs=(vmem, vmem, vmem, hbm, hbm),
            scratch_shapes=[space((SEQS, WIDTH), BF16), dma, dma],
            input_output_aliases={6: 1, 7: 2, 8: 3, 9: 4},
            compiler_params=pltpu.CompilerParams(vmem_limit_bytes=3 << 20),
        )(positions, tokens, in_vmem(kv), in_vmem(rows_e), in_vmem(rows_l), in_vmem(wobuf), in_vmem(keep_k), in_vmem(keep_v), k_out, v_out)
        return block_out, k_out.reshape(k_cache.shape), v_out.reshape(v_cache.shape), new.reshape(SEQS, 2, KV, DIM)

    return jax.shard_map(device_step, mesh=mesh, in_specs=(P('dp', None), P('dp'), cache_spec, cache_spec, P(), P(), P(), P(), P(), P(), P()), out_specs=(P('dp', None), cache_spec, cache_spec, P('dp', None, None, None)), check_vma=False)
```

```python
import jax
import jax.numpy as jnp
import numpy as np
from jax import lax
from jax.experimental import pallas as pl
from jax.experimental.pallas import tpu as pltpu
from jax.sharding import PartitionSpec as P

NORM_EPS = 1e-6
ROPE_THETA = 1000000.0
NEG_FILL = -1e30
F32 = jnp.float32
BF16 = jnp.bfloat16
MESH = pl.DeviceIdType.MESH

SEQS = 64
WIDTH = 2048
HEADS = 16
KV = 8
DIM = 128
SLOTS = 256
ROWS = SLOTS * KV
RANKS = 8
OWN = SEQS // RANKS
EARLY = 48
LATE = SEQS - EARLY
OWN_E = EARLY // RANKS
OWN_L = LATE // RANKS
PART_E = OWN_E * HEADS + 8
PART_L = OWN_L * HEADS + 8
CHUNK = 512
RING = 16
PAIRS = RING // 2
LAG = 3
COLS = 512
CHUNKS = WIDTH // COLS


def frequencies():
    half = ROPE_THETA ** (-np.arange(DIM // 2, dtype=np.float64) * 2.0 / DIM)
    return jnp.asarray(np.concatenate([half, half])[None, :], F32)


def head_columns():
    row = lax.broadcasted_iota(jnp.int32, (HEADS, ROWS), 0)
    col = lax.broadcasted_iota(jnp.int32, (HEADS, ROWS), 1)
    return jnp.where((col & (KV - 1)) == (row >> 1), col, 1 << 30)


def insert(buf, index, local, new):
    row = lax.broadcasted_iota(jnp.int32, (2 * KV, DIM), 0)
    slot = jnp.clip(local, 0, SLOTS - 1)
    first = jnp.where(local == slot, (slot & 1) * KV, 64)
    block = pl.ds(pl.multiple_of((slot >> 1) * 2 * KV, 2 * KV), 2 * KV)
    both = jnp.concatenate([new, new], axis=0)
    old = buf[index, block, :].astype(F32)
    hit = (row >= first) & (row < first + KV)
    buf[index, block, :] = jnp.where(hit, both, old).astype(BF16)


def scores_of(q, k):
    return lax.dot_general(q, k, (((1,), (1,)), ((), ())), preferred_element_type=F32) * (DIM ** -0.5)


def stat_tile(peak, total):
    lane = lax.broadcasted_iota(jnp.int32, (HEADS, DIM), 1)
    return jnp.where(lane == 0, peak, total)


def early_kernel(pos_ref, tok_ref, freq_ref, an_ref, qn_ref, kn_ref, wq_ref, wk_ref, wv_ref, k_ref, v_ref,
                 part_ref, q_scr, kv_scr, new_ref, ko_ref, vo_ref,
                 wbuf, hid, cos_scr, sin_scr, key, stat, kbuf, vbuf, wsem, krs, vrs, kws, vws):
    start = lax.axis_index('sp') * SLOTS

    def weight_copy(c):
        if c < 4:
            src = wq_ref.at[:, pl.ds(c * CHUNK, CHUNK)]
        elif c < 6:
            src = wk_ref.at[:, pl.ds((c - 4) * CHUNK, CHUNK)]
        else:
            src = wv_ref.at[:, pl.ds((c - 6) * CHUNK, CHUNK)]
        return pltpu.make_async_copy(src, wbuf.at[c], wsem.at[c])

    def pair_slots(i):
        return pl.ds(2 * lax.rem(i, PAIRS), 2)

    def reads(i):
        s = lax.rem(i, PAIRS)
        return (pltpu.make_async_copy(k_ref.at[pl.ds(2 * i, 2)], kbuf.at[pair_slots(i)], krs.at[s]),
                pltpu.make_async_copy(v_ref.at[pl.ds(2 * i, 2)], vbuf.at[pair_slots(i)], vrs.at[s]))

    def writes(i):
        s = lax.rem(i, PAIRS)
        return (pltpu.make_async_copy(kbuf.at[pair_slots(i)], ko_ref.at[pl.ds(2 * i, 2)], kws.at[s]),
                pltpu.make_async_copy(vbuf.at[pair_slots(i)], vo_ref.at[pl.ds(2 * i, 2)], vws.at[s]))

    for c in range(8):
        weight_copy(c).start()

    def first_reads(i, carry):
        for copy in reads(i):
            copy.start()
        return carry

    lax.fori_loop(0, PAIRS, first_reads, 0)

    x = tok_ref[...].astype(F32)
    scale = lax.rsqrt(jnp.mean(x * x, axis=-1, keepdims=True) + NORM_EPS)
    hid[...] = (x * scale * an_ref[...].astype(F32)[None, :]).astype(BF16)

    def fill(b, carry):
        cos_scr[pl.ds(b, 1), :] = jnp.full((1, DIM), pos_ref[b].astype(F32), F32)
        return carry

    lax.fori_loop(0, SEQS, fill, 0)
    angle = cos_scr[...] * freq_ref[...]
    lane = lax.broadcasted_iota(jnp.int32, (SEQS, DIM), 1)
    sin = jnp.sin(angle)
    cos_scr[...] = jnp.cos(angle)
    sin_scr[...] = jnp.where(lane < DIM // 2, -sin, sin)
    key[...] = head_columns()

    def norm_rope(y, gain):
        y = y * lax.rsqrt(jnp.mean(y * y, axis=-1, keepdims=True) + NORM_EPS) * gain
        return (y * cos_scr[...] + pltpu.roll(y, DIM // 2, 1) * sin_scr[...]).astype(BF16).astype(F32)

    qg = qn_ref[...].astype(F32)[None, :]
    kg = kn_ref[...].astype(F32)[None, :]
    for c in range(8):
        weight_copy(c).wait()
        y = jnp.dot(hid[...], wbuf[c], preferred_element_type=F32).astype(BF16).astype(F32)
        for j in range(CHUNK // DIM):
            yh = y[:, j * DIM:(j + 1) * DIM]
            if c < 4:
                q_scr[pl.ds(c * 4 + j, SEQS, stride=HEADS), :] = norm_rope(yh, qg)
            elif c < 6:
                kv_scr[pl.ds((c - 4) * 4 + j, SEQS, stride=2 * KV), :] = norm_rope(yh, kg)
            else:
                kv_scr[pl.ds(KV + (c - 6) * 4 + j, SEQS, stride=2 * KV), :] = yh
    new_ref[...] = kv_scr[...].astype(BF16)

    def attend(b):
        s = lax.rem(b, RING)
        local = pos_ref[b] - start
        q = q_scr[pl.ds(pl.multiple_of(b * HEADS, HEADS), HEADS), :].astype(BF16)
        scores = scores_of(q, kbuf[s])
        live = key[...] < (local + 1) * KV
        scores = jnp.where(live, scores, NEG_FILL)
        peak = jnp.max(scores, axis=-1, keepdims=True)
        e = jnp.where(live, jnp.exp(scores - peak), 0.0)
        total = jnp.sum(e, axis=-1, keepdims=True)
        out = jnp.dot(e.astype(BF16), vbuf[s], preferred_element_type=F32)
        return out, stat_tile(peak, total)

    def group(g, carry):
        def pair(j, carry):
            i = g * (OWN_E // 2) + j
            b0 = 2 * i

            @pl.when(i >= LAG)
            def _():
                for copy in writes(i - LAG):
                    copy.wait()

            @pl.when((i >= LAG) & (i - LAG + PAIRS < EARLY // 2))
            def _():
                for copy in reads(i - LAG + PAIRS):
                    copy.start()

            for copy in reads(i):
                copy.wait()
            for d in range(2):
                b = b0 + d
                s = lax.rem(b, RING)
                local = pos_ref[b] - start
                base = pl.multiple_of(b * 2 * KV, 2 * KV)
                insert(kbuf, s, local, kv_scr[pl.ds(base, KV), :])
                insert(vbuf, s, local, kv_scr[pl.ds(pl.multiple_of(base + KV, KV), KV), :])
            for d in range(2):
                out, st = attend(b0 + d)
                r = pl.multiple_of((2 * j + d) * HEADS, HEADS)
                part_ref[g, pl.ds(r, HEADS), :] = out
                stat[pl.ds(r, HEADS), :] = st
            for copy in writes(i):
                copy.start()
            return carry

        lax.fori_loop(0, OWN_E // 2, pair, 0)
        part_ref[g, pl.ds(OWN_E * HEADS, 8), pl.ds(0, OWN_E * HEADS)] = stat[...].T[0:8, :]
        return carry

    lax.fori_loop(0, RANKS, group, 0)
    for i in range(EARLY // 2 - LAG, EARLY // 2):
        for copy in writes(i):
            copy.wait()


def bit(value, place):
    if isinstance(value, int):
        return value // place % 2
    return lax.rem(lax.div(value, place), 2)


def flip(index, mask):
    return sum(lax.rem(bit(index, p) + bit(mask, p), 2) * p for p in (1, 2, 4))


def late_sequence(me, n):
    return EARLY + flip(me, RANKS - 1 - lax.div(n, OWN_L)) * OWN_L + lax.rem(n, OWN_L)


def late_kernel(pos_ref, q_ref, kv_ref, early_ref, wo_ref, k_ref, v_ref,
                out_e, out_l, wobuf, keep_k, keep_v,
                key, stat, late, recv_e, recv_l, own_e, own_l,
                wsem, krs, vrs, es, er, ls, lr, ges, ger, gls, glr):
    me = lax.axis_index('sp')
    start = me * SLOTS

    def reads(i):
        b = late_sequence(me, 2 * i)
        return (pltpu.make_async_copy(k_ref.at[pl.ds(b, 2)], keep_k.at[pl.ds(2 * i, 2)], krs.at[i]),
                pltpu.make_async_copy(v_ref.at[pl.ds(b, 2)], keep_v.at[pl.ds(2 * i, 2)], vrs.at[i]))

    def wo_copy(c):
        return pltpu.make_async_copy(wo_ref.at[:, pl.ds(pl.multiple_of(c * COLS, COLS), COLS)], wobuf.at[c], wsem.at[c])

    def remote(src, dst, send, recv, mask):
        return pltpu.make_async_remote_copy(src_ref=src, dst_ref=dst, send_sem=send, recv_sem=recv,
                                            device_id={'sp': flip(me, mask)}, device_id_type=MESH)

    def early_copy(m):
        return remote(early_ref.at[flip(me, m)], recv_e.at[m], es.at[m], er.at[m], m)

    def late_copy(m):
        return remote(late.at[m], recv_l.at[m], ls.at[m], lr.at[m], m)

    def start_reads(n, carry):
        for copy in reads(n):
            copy.start()
        return carry

    lax.fori_loop(0, 2, start_reads, 0)

    barrier = pltpu.get_barrier_semaphore()
    for m in range(1, RANKS):
        pl.semaphore_signal(barrier, inc=1, device_id={'sp': flip(me, m)}, device_id_type=MESH)
    pl.semaphore_wait(barrier, RANKS - 1)
    for m in range(RANKS - 1, 0, -1):
        early_copy(m).start()
    lax.fori_loop(2, LATE // 2, start_reads, 0)
    recv_e[0] = early_ref[me]
    key[...] = head_columns()

    row16 = lax.broadcasted_iota(jnp.int32, (HEADS, 2 * KV), 0)
    col16 = lax.broadcasted_iota(jnp.int32, (HEADS, 2 * KV), 1)

    def attend(n):
        b = late_sequence(me, n)
        local = pos_ref[b] - start
        base = pl.ds(pl.multiple_of(b * HEADS, HEADS), HEADS)
        q = q_ref[base, :].astype(BF16)
        kv = kv_ref[base, :].astype(BF16)
        scores = scores_of(q, keep_k[n])
        live = key[...] < local * KV
        scores = jnp.where(live, scores, NEG_FILL)
        mine = jnp.where((local >= 0) & (local < SLOTS), row16 >> 1, 64)
        fresh = jnp.where(col16 == mine, scores_of(q, kv), NEG_FILL)
        fresh = jnp.max(fresh, axis=-1, keepdims=True)
        peak = jnp.maximum(jnp.max(scores, axis=-1, keepdims=True), fresh)
        e = jnp.where(live, jnp.exp(scores - peak), 0.0)
        ef = jnp.where(col16 == mine + KV, jnp.exp(fresh - peak), 0.0)
        total = jnp.sum(e, axis=-1, keepdims=True) + jnp.sum(ef, axis=-1, keepdims=True)
        out = jnp.dot(e.astype(BF16), keep_v[n], preferred_element_type=F32)
        out = out + jnp.dot(ef.astype(BF16), kv, preferred_element_type=F32)
        return out, stat_tile(peak, total)

    def group(g, carry):
        m = RANKS - 1 - g

        def pair(j, carry):
            n0 = g * OWN_L + 2 * j

            for copy in reads(g * (OWN_L // 2) + j):
                copy.wait()
            for d in range(2):
                out, st = attend(n0 + d)
                r = pl.multiple_of((2 * j + d) * HEADS, HEADS)
                late[m, pl.ds(r, HEADS), :] = out
                stat[pl.ds(r, HEADS), :] = st
            return carry

        lax.fori_loop(0, OWN_L // 2, pair, 0)
        late[m, pl.ds(OWN_L * HEADS, 8), pl.ds(0, OWN_L * HEADS)] = stat[...].T[0:8, :]

        @pl.when(g + 1 < RANKS)
        def _():
            late_copy(m).start()

        return carry

    def combine(recv, count):
        rows = count * HEADS
        stats = [recv[s, pl.ds(rows, 8), pl.ds(0, rows)].T for s in range(RANKS)]
        peak = stats[0][:, 0:1]
        for s in range(1, RANKS):
            peak = jnp.maximum(peak, stats[s][:, 0:1])
        total = jnp.zeros((rows, 1), F32)
        acc = jnp.zeros((rows, DIM), F32)
        for s in range(RANKS):
            w = jnp.exp(stats[s][:, 0:1] - peak)
            total = total + w * stats[s][:, 1:2]
            acc = acc + w * recv[s, pl.ds(0, rows), :]
        return acc / total

    def gather(own, out, gs, gr, relayed):
        direct = (6, 4, 2, 1) if relayed else (7, 6, 5, 4, 3, 2, 1)
        through = (2, 4, 6) if relayed else ()
        rest = (1, 3, 5, 7) if relayed else direct
        size = own.shape[0]

        def place(rank):
            return out.at[pl.ds(pl.multiple_of(rank * size, size), size), :]

        def send(mask):
            return remote(own, place(me), gs.at[mask], gr.at[me], mask)

        def relay(mask):
            src = flip(me, mask)
            return remote(place(src), place(src), gs.at[mask + 1], gr.at[src], 1)

        def arrival(mask):
            src = flip(me, mask)
            return remote(own, place(src), gs.at[mask], gr.at[src], mask)

        def first():
            for mask in direct:
                send(mask).start()
            out[pl.ds(pl.multiple_of(me * size, size), size), :] = own[...]

        def second():
            for mask in through:
                arrival(mask).wait_recv()
                relay(mask).start()

        def last():
            for mask in rest:
                arrival(mask).wait_recv()
            for mask in direct:
                send(mask).wait_send()
            for mask in through:
                relay(mask).wait_send()

        return first, second, last

    stages_e = gather(own_e, out_e, ges, ger, True)
    stages_l = gather(own_l, out_l, gls, glr, False)
    lax.fori_loop(0, RANKS - 1, group, 0)
    for m in range(RANKS - 1, 0, -1):
        early_copy(m).wait()
    own_e[...] = combine(recv_e, OWN_E)
    stages_e[0]()
    for c in range(CHUNKS // 2):
        wo_copy(c).start()
    lax.fori_loop(RANKS - 1, RANKS, group, 0)
    recv_l[0] = late[0]
    for m in range(RANKS - 1, 0, -1):
        late_copy(m).wait()
    own_l[...] = combine(recv_l, OWN_L)
    stages_l[0]()
    for c in range(CHUNKS // 2, CHUNKS):
        wo_copy(c).start()
    stages_e[1]()
    stages_l[1]()
    for c in range(CHUNKS):
        wo_copy(c).wait()
    stages_e[2]()
    stages_l[2]()


def store_kernel(pos_ref, tok_ref, kv_ref, rows_e, rows_l, wobuf, keep_k_in, keep_v_in, ko_in, vo_in,
                 out_ref, keep_k, keep_v, ko_ref, vo_ref, attn, kws, vws):
    me = lax.axis_index('sp')
    start = me * SLOTS

    def writes(i):
        b = late_sequence(me, 2 * i)
        return (pltpu.make_async_copy(keep_k.at[pl.ds(2 * i, 2)], ko_ref.at[pl.ds(b, 2)], kws),
                pltpu.make_async_copy(keep_v.at[pl.ds(2 * i, 2)], vo_ref.at[pl.ds(b, 2)], vws))

    def step(n, carry):
        b = late_sequence(me, jnp.minimum(n, LATE - 1))
        local = pos_ref[b] - start

        @pl.when((n < LATE) & (local >= 0) & (local < SLOTS))
        def _():
            base = pl.multiple_of(b * 2 * KV, 2 * KV)
            insert(keep_k, n, local, kv_ref[pl.ds(base, KV), :])
            insert(keep_v, n, local, kv_ref[pl.ds(pl.multiple_of(base + KV, KV), KV), :])

        @pl.when((n >= 3) & (lax.rem(n, 2) == 1))
        def _():
            for copy in writes(lax.div(n - 3, 2)):
                copy.start()

        return carry

    lax.fori_loop(0, LATE + 2, step, 0)
    for h in range(HEADS):
        block = pl.ds(h * DIM, DIM)
        attn[pl.ds(0, EARLY), block] = rows_e[pl.ds(h, EARLY, stride=HEADS), :].astype(BF16)
        attn[pl.ds(EARLY, LATE), block] = rows_l[pl.ds(h, LATE, stride=HEADS), :].astype(BF16)
    for c in range(CHUNKS):
        block = pl.ds(c * COLS, COLS)
        y = jnp.dot(attn[...], wobuf[c], preferred_element_type=F32)
        out_ref[:, block] = (tok_ref[:, block].astype(F32) + y).astype(BF16)

    def drain(n, carry):
        for copy in writes(n):
            copy.wait()
        return carry

    lax.fori_loop(0, LATE // 2, drain, 0)


def solution(mesh):
    cache_spec = P('dp', 'sp', None, None)
    hbm = pl.BlockSpec(memory_space=pltpu.HBM)
    vmem = pl.BlockSpec(memory_space=pltpu.VMEM)
    smem = pl.BlockSpec(memory_space=pltpu.SMEM)
    sds = jax.ShapeDtypeStruct
    flat = (SEQS, ROWS, DIM)
    dma = pltpu.SemaphoreType.DMA
    space = pltpu.VMEM

    def in_vmem(a):
        return pltpu.with_memory_space_constraint(a, pltpu.VMEM)

    def in_hbm(a):
        return pltpu.with_memory_space_constraint(a, pltpu.HBM)

    def device_step(tokens, positions, k_cache, v_cache, w_q, w_k, w_v, w_o, attn_norm, q_norm, k_norm):
        k_flat, v_flat = k_cache.reshape(flat), v_cache.reshape(flat)
        early, q, kv, new, k_out, v_out = pl.pallas_call(
            early_kernel,
            out_shape=(space((RANKS, PART_E, DIM), F32), space((SEQS * HEADS, DIM), F32), space((SEQS * 2 * KV, DIM), F32),
                       sds((SEQS * 2 * KV, DIM), BF16), sds(flat, BF16), sds(flat, BF16)),
            in_specs=[smem] + [vmem] * 5 + [hbm] * 5,
            out_specs=(vmem,) * 4 + (hbm,) * 2,
            scratch_shapes=[
                space((8, WIDTH, CHUNK), BF16), space((SEQS, WIDTH), BF16), space((SEQS, DIM), F32), space((SEQS, DIM), F32),
                space((HEADS, ROWS), jnp.int32), space((OWN_E * HEADS, DIM), F32),
                space((RING, ROWS, DIM), BF16), space((RING, ROWS, DIM), BF16),
                dma((8,)), dma((PAIRS,)), dma((PAIRS,)), dma((PAIRS,)), dma((PAIRS,)),
            ],
            compiler_params=pltpu.CompilerParams(vmem_limit_bytes=58 << 20),
        )(positions, tokens, frequencies(), attn_norm, q_norm, k_norm, in_hbm(w_q), in_hbm(w_k), in_hbm(w_v), in_hbm(k_flat), in_hbm(v_flat))
        rows_e, rows_l, wobuf, keep_k, keep_v = pl.pallas_call(
            late_kernel,
            out_shape=(space((EARLY * HEADS, DIM), F32), space((LATE * HEADS, DIM), F32), space((CHUNKS, WIDTH, COLS), BF16),
                       space((LATE, ROWS, DIM), BF16), space((LATE, ROWS, DIM), BF16)),
            in_specs=[smem] + [vmem] * 3 + [hbm] * 3,
            out_specs=(vmem,) * 5,
            scratch_shapes=[
                space((HEADS, ROWS), jnp.int32), space((OWN_L * HEADS, DIM), F32),
                space((RANKS, PART_L, DIM), F32), space((RANKS, PART_E, DIM), F32), space((RANKS, PART_L, DIM), F32),
                space((OWN_E * HEADS, DIM), F32), space((OWN_L * HEADS, DIM), F32),
                dma((CHUNKS,)), dma((LATE // 2,)), dma((LATE // 2,)), dma((RANKS,)), dma((RANKS,)), dma((RANKS,)), dma((RANKS,)),
                dma((RANKS,)), dma((RANKS,)), dma((RANKS,)), dma((RANKS,)),
            ],
            compiler_params=pltpu.CompilerParams(collective_id=0, has_side_effects=True, vmem_limit_bytes=3 << 20),
        )(positions, in_vmem(q), in_vmem(kv), in_vmem(early), in_hbm(w_o), in_hbm(k_flat), in_hbm(v_flat))
        block_out, _, _, k_out, v_out = pl.pallas_call(
            store_kernel,
            out_shape=(sds((SEQS, WIDTH), BF16), space((LATE, ROWS, DIM), BF16), space((LATE, ROWS, DIM), BF16), sds(flat, BF16), sds(flat, BF16)),
            in_specs=[smem] + [vmem] * 7 + [hbm] * 2,
            out_specs=(vmem, vmem, vmem, hbm, hbm),
            scratch_shapes=[space((SEQS, WIDTH), BF16), dma, dma],
            input_output_aliases={6: 1, 7: 2, 8: 3, 9: 4},
            compiler_params=pltpu.CompilerParams(vmem_limit_bytes=3 << 20),
        )(positions, tokens, in_vmem(kv), in_vmem(rows_e), in_vmem(rows_l), in_vmem(wobuf), in_vmem(keep_k), in_vmem(keep_v), k_out, v_out)
        return block_out, k_out.reshape(k_cache.shape), v_out.reshape(v_cache.shape), new.reshape(SEQS, 2, KV, DIM)

    return jax.shard_map(device_step, mesh=mesh, in_specs=(P('dp', None), P('dp'), cache_spec, cache_spec, P(), P(), P(), P(), P(), P(), P()), out_specs=(P('dp', None), cache_spec, cache_spec, P('dp', None, None, None)), check_vma=False)
```
